512 devices in a mesh: batch: 32 (over x, y), slab: 16 (over z, core).
Axes of the slice: x: 4, y: 8, z: 8, core: 2. Of those that a mesh axis runs over, the one named last changes fastest.
Arguments:
- volumes: float32 [64, 128, 128, 128], P('batch', 'slab'), may hold values from -6 to 6
- tilt_low: int32 [64], P('batch'), may hold values from -70 to -40
- tilt_high: int32 [64], P('batch'), may hold values from 40 to 70
- shifts: int32 [64, 3], P('batch'), may hold values from 0 to 127
- support: float32 [128, 128, 128], P('slab'), may hold values from 0.2 to 1
Outputs:
- average: float32 [128, 128, 128], P('slab')
- misfits: float32 [3], replicated
The draws below stay inside these ranges and needn't reach their ends.
Inputs may be any that keep to these rules, and one draw needn't show every extreme that they name: `shifts`: columns hold the shift along z, y and x.
All inputs are finite; a program needn't handle non-finite values.
Results may differ from the reference program's by a relative error of at most 0.0003.
Values sent between devices are 32-bit elements; how exact they have to be, the bound alone decides.
A program may use at most 64 MiB of HBM per device.

```python
import math
import jax
import jax.numpy as jnp
from jax import lax

N = 128
ITERS = 3
SUBS = 64


def with_ends(array, rng, smallest, top_value):
    index_at = [jax.random.randint(jax.random.fold_in(rng, axis), (), 0, length) for axis, length in enumerate(array.shape)]
    longest = array.shape.index(max(array.shape))
    next_to = index_at[:longest] + [(index_at[longest] + 1) % array.shape[longest]] + index_at[longest + 1:]
    return array.at[tuple(index_at)].set(smallest).at[tuple(next_to)].set(top_value)


def shard_levels(rng, shape, split, smallest, largest):
    def one(axis_at, shards_of):
        draws = jax.random.uniform(jax.random.fold_in(jax.random.fold_in(rng, 6), axis_at), (shards_of,), jnp.float32, smallest / len(split), largest / len(split))
        return jnp.repeat(jnp.exp(draws), shape[axis_at] // shards_of).reshape((-1,) + (1,) * (len(shape) - axis_at - 1))

    gain = one(*split[0])
    for cut in split[1:]:
        gain = gain * one(*cut)
    return gain


def bell_draw(own_key, extent, deviation, bound, shards=(), kind=jnp.bfloat16):
    loudness = shard_levels(own_key, extent, shards, -0.22, 0.18) if shards else 1.0
    result = jax.random.normal(own_key, extent, jnp.float32) * deviation * loudness
    return jnp.minimum(jnp.maximum(result, -bound), bound).astype(kind)


def setup_inputs(seed: int = 0) -> dict:
    streams_of = jax.random.split(jax.random.key(seed), 6)
    return {
        "volumes": bell_draw(streams_of[0], (SUBS, N, N, N), 1.0, 6.0, ((0, 32), (1, 16)), jnp.float32),
        "tilt_low": with_ends(jax.random.randint(streams_of[1], (SUBS,), -70, -39), jax.random.fold_in(streams_of[1], 1), -70, (-39) - 1).astype(jnp.int32),
        "tilt_high": with_ends(jax.random.randint(streams_of[2], (SUBS,), 40, 71), jax.random.fold_in(streams_of[2], 1), 40, 70).astype(jnp.int32),
        "shifts": with_ends(jax.random.randint(streams_of[3], (SUBS, 3), 0, N), jax.random.fold_in(streams_of[3], 1), 0, N - 1).astype(jnp.int32),
        "support": jnp.clip(0.2 + 0.8 * jax.random.uniform(streams_of[4], (N, N, N), jnp.float32) ** shard_levels(streams_of[4], (N, N, N), ((0, 16),), -0.2, 0.2), 0.2, 1.0),
    }


REG_WEIGHT = 0.5
FLOOR_VALUE = 1.0
SOFTNESS = 5.0
TO_DEGREES = 180.0 / math.pi


def signed(length):
    index = jnp.arange(length, dtype=jnp.int32)
    return jnp.where(index < length // 2, index, index - length)


def wedge(low, high, length):
    depth = signed(length)[:, None]
    across = signed(length)[None, :]
    facing = jnp.where(across >= 0, 1, -1)
    theta = jnp.arctan2((depth * facing).astype(jnp.float32), jnp.abs(across).astype(jnp.float32)) * TO_DEGREES
    lower = low.astype(jnp.float32)
    upper = high.astype(jnp.float32)
    return jax.nn.sigmoid((upper - theta) / SOFTNESS) * jax.nn.sigmoid((theta - lower) / SOFTNESS)


def spectrum(volume, offset):
    index = jnp.arange(N, dtype=jnp.int32)
    values = jnp.fft.fftn(volume, norm="ortho")
    turns = (index[:, None, None] * offset[0] + index[None, :, None] * offset[1] + index[None, None, :] * offset[2]) % N
    angle = turns.astype(jnp.float32) * (2.0 * math.pi / N)
    cosine = jnp.cos(angle)
    sine = jnp.sin(angle)
    return values.real * cosine + values.imag * sine, values.imag * cosine - values.real * sine


def reference(volumes, tilt_low, tilt_high, shifts, support):
    def gather_sums(carry, item):
        volume, low, high, offset = item
        weight = wedge(low, high, N)
        spread = weight[:, None, :]
        shifted_real, shifted_imag = spectrum(volume, offset)
        return (carry[0] + spread * shifted_real, carry[1] + spread * shifted_imag, carry[2] + weight * weight), None

    empty = jnp.zeros((N, N, N), jnp.float32)
    start = (empty, empty, jnp.zeros((N, N), jnp.float32))
    (sum_real, sum_imag, weight_sum), _ = lax.scan(gather_sums, start, (volumes, tilt_low, tilt_high, shifts))
    divisor_base = weight_sum[:, None, :]
    mean_real = empty
    mean_imag = empty
    misfits = []
    average = empty
    for turn in range(ITERS):
        def add_misfit(total, item):
            volume, low, high, offset = item
            spread = wedge(low, high, N)[:, None, :]
            shifted_real, shifted_imag = spectrum(volume, offset)
            diff_real = shifted_real - spread * mean_real
            diff_imag = shifted_imag - spread * mean_imag
            return total + jnp.sum(diff_real * diff_real + diff_imag * diff_imag), None

        total, _ = lax.scan(add_misfit, jnp.zeros((), jnp.float32), (volumes, tilt_low, tilt_high, shifts))
        mean_misfit = total / (SUBS * float(N * N * N))
        misfits.append(mean_misfit)
        damping = REG_WEIGHT * SUBS * mean_misfit + FLOOR_VALUE
        divisor = divisor_base + damping
        new_real = mean_real + (sum_real - divisor_base * mean_real) / divisor
        new_imag = mean_imag + (sum_imag - divisor_base * mean_imag) / divisor
        field = jnp.fft.ifftn(new_real + 1j * new_imag, norm="ortho").real
        average = support * field
        if turn + 1 < ITERS:
            values = jnp.fft.fftn(average, norm="ortho")
            mean_real = values.real
            mean_imag = values.imag
    return average, jnp.stack(misfits)
```

```python
import functools
import math

import jax
import jax.numpy as jnp
import numpy as np
from jax import lax
from jax.experimental import pallas as pl
from jax.experimental.pallas import tpu as pltpu
from jax.sharding import PartitionSpec as P

ITERS = 3
REG_WEIGHT = 0.5
FLOOR_VALUE = 1.0
SOFTNESS = 5.0
MESH = pl.DeviceIdType.MESH
LANES = 128
HALF = LANES // 2
XS = 4
GROUP = XS * 2
CHUNKS = 4
F32 = jnp.float32
BF16 = jnp.bfloat16


def signed(length):
    index = np.arange(length)
    return np.where(index < length // 2, index, index - length)


def tables(depth, width):
    half = depth // 2
    kz, z = np.arange(half), np.arange(depth)
    angle = 2 * np.pi * (kz[:, None] * z[None, :] % depth) / depth
    scale = 1 / math.sqrt(depth)
    down = np.zeros((depth + 8, depth))
    down[:half], down[half:depth] = np.cos(angle) * scale, -np.sin(angle) * scale
    down[depth] = np.where(z % 2 == 0, 1, -1) * scale
    twice = np.where(kz == 0, 1, 2)[None, :]
    up = np.concatenate([np.cos(angle.T) * twice, -np.sin(angle.T) * twice], 1) * scale
    kx = np.arange(width)
    turn = 2 * np.pi * (kx[:, None] * kx[None, :] % width) / width
    across = np.concatenate([np.cos(turn), np.sin(turn)], 1) / math.sqrt(width)
    fz, fx = signed(depth), signed(width)
    theta = np.degrees(np.arctan2(fz[:, None] * np.where(fx >= 0, 1, -1)[None, :], np.abs(fx)[None, :] * 1.0))
    mirror = theta[(-z) % depth][:, (-kx) % width]
    rows = np.minimum(np.arange(half + 8), half)
    theta, mirror = theta[rows], mirror[rows]
    mirror[0], mirror[half:] = theta[0], theta[half:]
    shift = 2 * np.pi * (rows[:, None] * np.arange(LANES)[None, :] % depth) / depth
    wedge = [np.exp(theta / SOFTNESS), np.exp(-theta / SOFTNESS), np.exp(mirror / SOFTNESS), np.exp(-mirror / SOFTNESS)]
    count = np.zeros((depth + 8, LANES))
    count[:depth], count[depth : depth + 2] = 2, 1
    count[0] = count[half] = 1
    single = np.concatenate(wedge + [np.cos(shift), np.sin(shift), count, np.cos(turn), np.sin(turn)], 0)
    return split(down), split(across), split(up), single.astype(np.float32)


def split(table):
    table = table.astype(np.float32)
    high = table.astype(BF16)
    low = (table - high.astype(np.float32)).astype(BF16)
    return np.concatenate([high, low], 0)


def halves(value):
    high = value.astype(BF16)
    return high, (value - high.astype(F32)).astype(BF16)


def mul(a, b):
    return jnp.dot(a, b, preferred_element_type=F32)


def by_table(value, table):
    rows = table.shape[0] // 2
    high, low = halves(value)
    top = table[:rows]
    return mul(high, top) + mul(low, top) + mul(high, table[rows:])


def table_by(table, value):
    rows = table.shape[0] // 2
    high, low = halves(value)
    top = table[:rows]
    return mul(top, high) + mul(top, low) + mul(table[rows:], high)


def arrange(slabs, v_ref, s_ref, shift_ref, u_ref, b_ref):
    ys = slabs * 8
    batch = lax.axis_index("batch")
    ring = lax.axis_size("batch") // XS
    mine = (batch // ring) * 2 + batch % 2
    energy = jnp.zeros((8, LANES), F32)
    for item in range(2):
        turn = shift_ref[item, 1]

        def block(t, energy, item=item, turn=turn):
            for k in range(8):
                y = lax.rem(t * 8 + k - turn + 2 * ys, ys)
                rows = v_ref[pl.ds(item * 8 * ys + y, 8, stride=ys), :]
                u_ref[t, k, item] = rows
                energy = energy + rows * rows
            return energy

        energy = lax.fori_loop(0, slabs, block, energy)

    def place(t, carry):
        b_ref[t, 0:8] = s_ref[pl.ds(t * 8 + mine, 8, stride=ys), :]
        b_ref[t, 8:16] = energy
        return carry

    lax.fori_loop(0, slabs, place, 0)


def refine(
    slabs, ring, u_ref, b_ref, t_ref, shift_ref, down, across, up, single, out_ref, mis_ref,
    block_in, tilt_out, tilt_in, tilts_out, tilts_in, rows_in, factors, part, parts_in, own_out, own_in,
    some_out, some_in, more_out, more_in, plane, pieces_in, planes_in,
    s_block, r_block, s_tilt, r_tilt, s_tilts, r_tilts, s_rows, r_rows, s_part, r_part, s_own, r_own,
    s_some, r_some, s_more, r_more, s_piece, r_piece, s_plane, r_plane,
):
    depth = slabs * 8
    half = depth // 2
    tall = half + 8
    copies = ring // 2
    subs = float(GROUP * copies * 2)
    cells = float(depth * depth * LANES)
    batch, slab = lax.axis_index("batch"), lax.axis_index("slab")
    x, y = batch // ring, batch % ring
    r, p = y // 2, y % 2
    g = x * 2 + p

    def at_slab(t):
        return (batch, t)

    def at_group(k):
        return ((k // 2) * ring + r * 2 + k % 2, slab)

    def at_copy(k):
        return (x * ring + k * 2 + p, slab)

    def each(count, me, act):
        def step(k, carry):
            off = count // 2 + (1 - k % 2) * (k // 2) - (k % 2) * ((k + 1) // 2)
            act(lax.rem(me + off, count))
            return carry

        if count > 1:
            lax.fori_loop(0, count - 1, step, 0)

    def exchange(count, me, device, source, target, send, recv):
        def copy(k, slot):
            return pltpu.make_async_remote_copy(
                src_ref=source(k), dst_ref=target(slot), send_sem=send.at[k], recv_sem=recv.at[slot],
                device_id=device(k), device_id_type=MESH,
            )

        return (
            lambda: each(count, me, lambda k: copy(k, me).start()),
            lambda: each(count, me, lambda k: copy(k, k).wait_recv()),
            lambda: each(count, me, lambda k: copy(k, me).wait_send()),
        )

    barrier = pltpu.get_barrier_semaphore()
    for count, me, device in ((slabs, slab, at_slab), (GROUP, g, at_group), (copies, r, at_copy)):
        each(count, me, lambda k, device=device: pl.semaphore_signal(
            barrier, inc=1, device_id=device(k), device_id_type=MESH))
    pl.semaphore_wait(barrier, slabs - 1 + GROUP - 1 + copies - 1)

    block = exchange(slabs, slab, at_slab, lambda k: b_ref.at[k], lambda k: block_in.at[k], s_block, r_block)
    tilt = exchange(GROUP, g, at_group, lambda k: tilt_out, lambda k: tilt_in.at[k], s_tilt, r_tilt)
    tilts = exchange(copies, r, at_copy, lambda k: tilts_out, lambda k: tilts_in.at[k], s_tilts, r_tilts)
    own = exchange(copies, r, at_copy, lambda k: own_out, lambda k: own_in.at[k], s_own, r_own)
    piece = exchange(
        slabs, slab, at_slab, lambda k: plane.at[pl.ds(pl.multiple_of(k * 8, 8), 8)], lambda k: pieces_in.at[k], s_piece, r_piece)
    whole = exchange(GROUP, g, at_group, lambda k: pieces_in, lambda k: planes_in.at[k], s_plane, r_plane)

    def chunk_rows(c):
        q = lax.rem(x + 1 + c, XS)
        return q, exchange(
            slabs, slab, at_slab, lambda k: u_ref.at[k, pl.ds(q * 2, 2)],
            lambda k: rows_in.at[pl.ds(q * 2, 2), :, k], s_rows.at[c], r_rows.at[c])

    def part_copy(k):
        return pltpu.make_async_remote_copy(
            src_ref=part.at[k], dst_ref=parts_in.at[g], send_sem=s_part.at[k], recv_sem=r_part.at[g],
            device_id=at_group(k), device_id_type=MESH)

    def part_wait(k):
        return pltpu.make_async_remote_copy(
            src_ref=part.at[k], dst_ref=parts_in.at[k], send_sem=s_part.at[k], recv_sem=r_part.at[k],
            device_id=at_group(k), device_id_type=MESH)

    block[0]()
    for c in range(2):
        chunk_rows(c)[1][0]()

    block_in[slab] = b_ref[slab]
    for k in range(8):
        for item in range(2):
            rows_in[k, item, slab] = u_ref[slab, k, item]

    lane = lax.broadcasted_iota(jnp.int32, (half, LANES), 1)
    row = lax.broadcasted_iota(jnp.int32, (half, LANES), 0)
    here = lane % HALF == row
    left = lane < HALF
    tile_row = lax.broadcasted_iota(jnp.int32, (8, LANES), 0)
    wide = lax.broadcasted_iota(jnp.int32, (tall, LANES), 1)

    def table(k):
        return single[k * tall : (k + 1) * tall]

    def weight(p_table, q_table, low, high):
        return 1.0 / ((1.0 + p_table * high) * (1.0 + q_table * low))

    for item in range(2):
        low, high = t_ref[0:1, item : item + 1], t_ref[0:1, item + 2 : item + 3]
        w = weight(table(0), table(1), low, high)
        dw = weight(table(2), table(3), low, high) - w
        pick = wide == shift_ref[item, 0]
        zc = jnp.sum(jnp.where(pick, table(4), 0.0), axis=1, keepdims=True)
        zs = jnp.sum(jnp.where(pick, table(5), 0.0), axis=1, keepdims=True)
        first = 6 * tall + depth + 8
        xc = single[pl.ds(first + shift_ref[item, 2], 1), :]
        xs = single[pl.ds(first + LANES + shift_ref[item, 2], 1), :]
        cosine, sine = zc * xc - zs * xs, zs * xc + zc * xs
        factors[item, 0], factors[item, 1] = w * cosine, w * sine
        factors[item, 2], factors[item, 3] = dw * cosine, dw * sine

    block[1]()
    energy = block_in[0, 8:16]
    for k in range(1, slabs):
        energy = energy + block_in[k, 8:16]
    tilt_out[0:8] = t_ref[...]
    tilt_out[8:16] = energy
    tilt[0]()
    tilt_in[g] = tilt_out[...]

    def chunk(c):
        q, rows = chunk_rows(c)
        rows[1]()
        stack = []
        for k in range(2):
            for item in range(2):
                stack.append(table_by(down, rows_in[q * 2 + k, item].reshape(depth, LANES)))
        product = by_table(jnp.concatenate(stack, 0), across)
        for k in range(2):
            re = im = re_last = im_last = d_re = d_im = 0.0
            for item in range(2):
                at = (k * 2 + item) * (depth + 8)
                c_top, c_low, c_last = (product[at + a : at + b, :LANES] for a, b in ((0, half), (half, depth), (depth, depth + 8)))
                s_top, s_low, s_last = (product[at + a : at + b, LANES:] for a, b in ((0, half), (half, depth), (depth, depth + 8)))
                a, b = c_top + s_low, c_low - s_top
                wc, ws = factors[item, 0, :half], factors[item, 1, :half]
                re, im = re + wc * a + ws * b, im + wc * b - ws * a
                wc, ws = factors[item, 2, :half], factors[item, 3, :half]
                d_re, d_im = d_re + wc * a + ws * b, d_im + wc * b - ws * a
                wc, ws = factors[item, 0, half:], factors[item, 1, half:]
                re_last, im_last = re_last + wc * c_last - ws * s_last, im_last - wc * s_last - ws * c_last

            def lying(d):
                column = jnp.where(left, d[:, 0:1], d[:, HALF : HALF + 1])
                return jnp.sum(jnp.where(here, column, 0.0), axis=0, keepdims=True)

            last = jnp.where(tile_row == 0, re_last[0:1], jnp.where(tile_row == 1, im_last[0:1], 0.0))
            last = jnp.where(tile_row == 2, lying(d_re), jnp.where(tile_row == 3, lying(d_im), last))
            part[q * 2 + k, 0:half], part[q * 2 + k, half:depth] = re, im
            part[q * 2 + k, depth:] = last
        return q

    def add_up(ref, count):
        total = ref[0]
        for k in range(1, count):
            total = total + ref[k]
        return total

    for c in range(CHUNKS):
        q = chunk(c)
        if c < CHUNKS - 1:
            part_copy(q * 2 + (1 - p)).start()
            part_copy(q * 2 + p).start()
        else:
            part_copy(q * 2 + (1 - p)).start()
        if c + 2 < CHUNKS:
            chunk_rows(c + 2)[1][0]()
        if c == 0:
            tilt[1]()
            tilts_out[0:8] = jnp.concatenate([tilt_in[k, 0:1] for k in range(GROUP)], 0)
            energy = tilt_in[0, 8:16]
            for k in range(1, GROUP):
                energy = energy + tilt_in[k, 8:16]
            tilts_out[8:16] = energy
            tilts[0]()
            tilts_in[r] = tilts_out[...]
        if c == 2:
            tilts[1]()
            energy = tilts_in[0, 8:16]
            for k in range(1, copies):
                energy = energy + tilts_in[k, 8:16]

            def square(k, totals):
                total, mirrored = totals
                for j in range(GROUP):
                    for item in range(2):
                        low, high = tilts_in[k, j : j + 1, item : item + 1], tilts_in[k, j : j + 1, item + 2 : item + 3]
                        w = weight(table(0), table(1), low, high)
                        total = total + w * w
                        w = weight(table(2), table(3), low, high)
                        mirrored = mirrored + w * w
                return total, mirrored

            none = jnp.zeros((tall, LANES), F32)
            total, mirrored = lax.fori_loop(0, copies, square, (none, none))

    parts_in[g] = part[g]
    each(GROUP, g, lambda k: part_wait(k).wait_recv())
    own_out[...] = add_up(parts_in, GROUP)
    own[0]()
    own_in[r] = own_out[...]

    def stacked(d):
        return jnp.concatenate([d[:half], d[:half], jnp.where(tile_row < 2, d[half : half + 1], 0.0)], 0)

    d_one, d_two = stacked(total), stacked(mirrored)
    support = block_in[:, 0:8].reshape(depth, LANES)
    sign = jnp.where(lax.broadcasted_iota(jnp.int32, (depth, LANES), 0) % 2 == 0, 1.0, -1.0) * (1 / math.sqrt(depth))
    count = single[6 * tall : 6 * tall + depth + 8]
    own[1]()
    sums = add_up(own_in, copies)

    def standing(values):
        spread = jnp.where(here, values, 0.0)
        one = jnp.sum(jnp.where(left, spread, 0.0), axis=1, keepdims=True)
        two = jnp.sum(jnp.where(left, 0.0, spread), axis=1, keepdims=True)
        return jnp.where(lane == 0, one, jnp.where(lane == HALF, two, 0.0))

    change = jnp.concatenate(
        [standing(sums[depth + 2 : depth + 3]), standing(sums[depth + 3 : depth + 4]), jnp.zeros((8, LANES), F32)], 0)
    sums = jnp.concatenate([sums[:depth], jnp.where(tile_row < 2, sums[depth:], 0.0)], 0)
    mean = jnp.zeros((depth + 8, LANES), F32)
    power = jnp.sum(energy, axis=(0, 1), keepdims=True)
    misfit = power * (1.0 / (subs * cells))
    misfits = jnp.where(tile_row == 0, misfit, 0.0)
    for turn in range(ITERS):
        damping = REG_WEIGHT * subs * misfit + FLOOR_VALUE
        one, two = 0.5 / (d_one + damping), 0.5 / (d_two + damping)
        update = mean - mean * (d_one * one + d_two * two) + (one + two) * sums + two * change
        product = by_table(update, across)
        re = product[:half, :LANES] - product[half:depth, LANES:]
        im = product[half:depth, :LANES] + product[:half, LANES:]
        last = product[depth : depth + 1, :LANES] - product[depth + 1 : depth + 2, LANES:]
        average = support * (table_by(up, jnp.concatenate([re, im], 0)) + sign * last)
        if turn + 1 == ITERS:
            break
        product = by_table(table_by(down, average), across)
        last = jnp.where(tile_row == 0, product[depth : depth + 1, :LANES], -product[depth : depth + 1, LANES:])
        mean = jnp.concatenate([
            product[:half, :LANES] + product[half:depth, LANES:],
            product[half:depth, :LANES] - product[:half, LANES:],
            jnp.where(tile_row < 2, last, 0.0)], 0)
        terms = count * mean * (0.5 * (d_one + d_two) * mean - 2.0 * sums - change)
        some_out[turn] = jnp.sum(terms.reshape(depth // 8 + 1, 8, LANES), axis=0)
        some = exchange(
            GROUP, g, at_group, lambda k: some_out.at[turn], lambda k: some_in.at[turn, k], s_some.at[turn], r_some.at[turn])
        some[0]()
        some_in[turn, g] = some_out[turn]
        some[1]()
        more_out[turn] = add_up(some_in.at[turn], GROUP)
        more = exchange(
            slabs, slab, at_slab, lambda k: more_out.at[turn], lambda k: more_in.at[turn, k], s_more.at[turn], r_more.at[turn])
        more[0]()
        more_in[turn, slab] = more_out[turn]
        more[1]()
        misfit = (power + jnp.sum(add_up(more_in.at[turn], slabs), axis=(0, 1), keepdims=True)) * (1.0 / (subs * cells))
        misfits = jnp.where(tile_row == turn + 1, misfit, misfits)
        some[2]()
        more[2]()
    mis_ref[...] = misfits
    plane[...] = average
    piece[0]()
    pieces_in[slab] = plane[pl.ds(pl.multiple_of(slab * 8, 8), 8)]
    piece[1]()
    whole[0]()

    def place(k, source):
        for j in range(slabs):
            out_ref[pl.ds(j * 8 + k, 8, stride=depth), :] = source[j]

    place(g, pieces_in)
    block[2](), tilt[2](), tilts[2](), own[2](), piece[2]()
    for c in range(CHUNKS):
        chunk_rows(c)[1][2]()
    each(GROUP, g, lambda k: part_wait(k).wait_send())
    whole[1]()
    each(GROUP, g, lambda k: place(k, planes_in.at[k]))
    whole[2]()


def body(volumes, tilt_low, tilt_high, shifts, support):
    slabs, ring = lax.axis_size("slab"), lax.axis_size("batch") // XS
    layer, ys, width = support.shape
    depth, copies, tall = layer * slabs, ring // 2, slabs * 8 + 8
    vmem, smem = pl.BlockSpec(memory_space=pltpu.VMEM), pl.BlockSpec(memory_space=pltpu.SMEM)
    u, blocks = pl.pallas_call(
        functools.partial(arrange, slabs),
        out_shape=(
            jax.ShapeDtypeStruct((slabs, 8, 2, 8, LANES), F32),
            jax.ShapeDtypeStruct((slabs, 16, LANES), F32),
        ),
        in_specs=[vmem, vmem, smem],
        out_specs=(vmem, vmem),
        name="arrange",
    )(volumes.reshape(2 * layer * ys, width), support.reshape(layer * ys, width), shifts)
    edges = jnp.concatenate(
        [jnp.exp(tilt_low.astype(F32) / SOFTNESS), jnp.exp(-tilt_high.astype(F32) / SOFTNESS)])
    edges = jnp.pad(edges[None, :], ((0, 7), (0, LANES - 4)))
    dma = pltpu.SemaphoreType.DMA

    def buffer(*shape):
        return pltpu.VMEM((*shape, LANES), F32)

    average, misfits = pl.pallas_call(
        functools.partial(refine, slabs, ring),
        out_shape=(
            jax.ShapeDtypeStruct((layer * ys, width), F32),
            jax.ShapeDtypeStruct((8, LANES), F32),
        ),
        in_specs=[vmem, vmem, vmem, smem, vmem, vmem, vmem, vmem],
        out_specs=(vmem, vmem),
        scratch_shapes=[
            buffer(slabs, 16), buffer(16), buffer(GROUP, 16), buffer(16), buffer(copies, 16),
            buffer(8, 2, slabs, 8), buffer(2, 4, depth // 2 + 8),
            buffer(GROUP, tall), buffer(GROUP, tall), buffer(tall), buffer(copies, tall),
            buffer(2, 8), buffer(2, GROUP, 8), buffer(2, 8), buffer(2, slabs, 8),
            buffer(depth), buffer(slabs, 8), buffer(GROUP, slabs, 8),
            dma((slabs,)), dma((slabs,)), dma((GROUP,)), dma((GROUP,)), dma((copies,)), dma((copies,)),
            dma((CHUNKS, slabs)), dma((CHUNKS, slabs)), dma((GROUP,)), dma((GROUP,)), dma((copies,)), dma((copies,)),
            dma((2, GROUP)), dma((2, GROUP)), dma((2, slabs)), dma((2, slabs)),
            dma((slabs,)), dma((slabs,)), dma((GROUP,)), dma((GROUP,)),
        ],
        compiler_params=pltpu.CompilerParams(collective_id=0, has_side_effects=True),
        name="refine",
    )(u, blocks, edges, shifts, *(jnp.asarray(t) for t in tables(depth, width)))
    return average.reshape(layer, ys, width), misfits[:ITERS, 0]


def solution(mesh):
    placed = (
        P("batch", "slab", None, None),
        P("batch"),
        P("batch"),
        P("batch", None),
        P("slab", None, None),
    )
    return jax.shard_map(
        body, mesh=mesh, in_specs=placed, out_specs=(P("slab", None, None), P()), check_vma=False
    )
```

```python
import functools
import math

import jax
import jax.numpy as jnp
import numpy as np
from jax import lax
from jax.experimental import pallas as pl
from jax.experimental.pallas import tpu as pltpu
from jax.sharding import PartitionSpec as P

ITERS = 3
REG_WEIGHT = 0.5
FLOOR_VALUE = 1.0
SOFTNESS = 5.0
MESH = pl.DeviceIdType.MESH
LANES = 128
HALF = LANES // 2
XS = 4
GROUP = XS * 2
CHUNKS = 5
F32 = jnp.float32
BF16 = jnp.bfloat16


def signed(length):
    index = np.arange(length)
    return np.where(index < length // 2, index, index - length)


def tables(depth, width):
    half = depth // 2
    kz, z = np.arange(half), np.arange(depth)
    angle = 2 * np.pi * (kz[:, None] * z[None, :] % depth) / depth
    scale = 1 / math.sqrt(depth)
    down = np.zeros((depth + 8, depth))
    down[:half], down[half:depth] = np.cos(angle) * scale, -np.sin(angle) * scale
    down[depth] = np.where(z % 2 == 0, 1, -1) * scale
    twice = np.where(kz == 0, 1, 2)[None, :]
    up = np.concatenate([np.cos(angle.T) * twice, -np.sin(angle.T) * twice], 1) * scale
    kx = np.arange(width)
    turn = 2 * np.pi * (kx[:, None] * kx[None, :] % width) / width
    across = np.concatenate([np.cos(turn), np.sin(turn)], 1) / math.sqrt(width)
    fz, fx = signed(depth), signed(width)
    theta = np.degrees(np.arctan2(fz[:, None] * np.where(fx >= 0, 1, -1)[None, :], np.abs(fx)[None, :] * 1.0))
    mirror = theta[(-z) % depth][:, (-kx) % width]
    rows = np.minimum(np.arange(half + 8), half)
    theta, mirror = theta[rows], mirror[rows]
    mirror[0], mirror[half:] = theta[0], theta[half:]
    shift = 2 * np.pi * (rows[:, None] * np.arange(LANES)[None, :] % depth) / depth
    wedge = [np.exp(theta / SOFTNESS), np.exp(-theta / SOFTNESS), np.exp(mirror / SOFTNESS), np.exp(-mirror / SOFTNESS)]
    count = np.zeros((depth + 8, LANES))
    count[:depth], count[depth : depth + 2] = 2, 1
    count[0] = count[half] = 1
    single = np.concatenate(wedge + [np.cos(shift), np.sin(shift), count, np.cos(turn), np.sin(turn)], 0)
    return split(down), split(across), split(up), single.astype(np.float32)


def split(table):
    table = table.astype(np.float32)
    high = table.astype(BF16)
    low = (table - high.astype(np.float32)).astype(BF16)
    return np.concatenate([high, low], 0)


def halves(value):
    high = value.astype(BF16)
    return high, (value - high.astype(F32)).astype(BF16)


def mul(a, b):
    return jnp.dot(a, b, preferred_element_type=F32)


def by_table(value, table):
    rows = table.shape[0] // 2
    high, low = halves(value)
    top = table[:rows]
    return mul(high, top) + mul(low, top) + mul(high, table[rows:])


def table_by(table, value):
    rows = table.shape[0] // 2
    high, low = halves(value)
    top = table[:rows]
    return mul(top, high) + mul(top, low) + mul(table[rows:], high)


def refine(
    slabs, ring, v_hbm, s_hbm, down_hbm, across_hbm, up_hbm, single_hbm, low_ref, high_ref, shift_ref, out_ref, mis_ref,
    v_ref, s_ref, down_ref, across_ref, up_ref, single, u_ref, blocks,
    power_out, power_in, block_in, tilt_out, tilt_in, tilts_out, tilts_in, rows_in, factors, part, parts_in, own_out, own_in,
    some_out, some_in, more_out, more_in, plane, pieces_in, planes_in, s_load, s_volume,
    s_power, r_power, s_block, r_block, s_tilt, r_tilt, s_tilts, r_tilts, s_rows, r_rows, s_part, r_part, s_own, r_own,
    s_some, r_some, s_more, r_more, s_piece, r_piece, s_plane, r_plane,
):
    depth = slabs * 8
    half = depth // 2
    tall = half + 8
    copies = ring // 2
    subs = float(GROUP * copies * 2)
    cells = float(depth * depth * LANES)
    batch, slab = lax.axis_index("batch"), lax.axis_index("slab")
    x, y = batch // ring, batch % ring
    r, p = y // 2, y % 2
    g = x * 2 + p

    def at_slab(t):
        return (batch, t)

    def at_group(k):
        return (lax.div(k, 2) * ring + r * 2 + lax.rem(k, 2), slab)

    def at_copy(k):
        return (x * ring + k * 2 + p, slab)

    def each(count, me, act, unroll=True):
        if unroll:
            for off in sorted(range(1, count), key=lambda off: abs(off - count / 2)):
                act(lax.rem(me + off, count))
            return

        def step(k, carry):
            act(lax.rem(me + 1 + lax.rem(k + count // 4, count - 1), count))
            return carry

        if count > 1:
            lax.fori_loop(0, count - 1, step, 0)

    def exchange(count, me, device, source, target, send, recv, unroll=True):
        def copy(k, slot):
            return pltpu.make_async_remote_copy(
                src_ref=source(k), dst_ref=target(slot), send_sem=send.at[k], recv_sem=recv.at[slot],
                device_id=device(k), device_id_type=MESH,
            )

        return (
            lambda: each(count, me, lambda k: copy(k, me).start(), unroll),
            lambda: each(count, me, lambda k: copy(k, k).wait_recv(), unroll),
            lambda: each(count, me, lambda k: copy(k, me).wait_send(), False),
        )

    barrier = pltpu.get_barrier_semaphore()
    for count, me, device in ((slabs, slab, at_slab), (GROUP, g, at_group), (copies, r, at_copy)):
        each(count, me, lambda k, device=device: pl.semaphore_signal(
            barrier, inc=1, device_id=device(k), device_id_type=MESH))
    def volume_copy(k, again):
        return pltpu.make_async_copy(
            v_hbm.at[k], v_ref.at[pl.ds(pl.multiple_of(2 * depth * k + depth * again, depth), depth)], s_volume.at[again, k])

    loads = [
        pltpu.make_async_copy(source, target, s_load.at[k])
        for k, (source, target) in enumerate((
            (s_hbm, s_ref), (single_hbm, single), (down_hbm, down_ref), (across_hbm, across_ref), (up_hbm, up_ref)))
    ]

    def over(count, act):
        def step(k, carry):
            act(k)
            return carry

        lax.fori_loop(0, count, step, 0)

    for again in range(2):
        over(16, lambda k, again=again: volume_copy(k, again).start())
    for load in loads:
        load.start()
    for again in range(2):
        over(16, lambda k, again=again: volume_copy(k, again).wait())
    power = jnp.zeros((8, LANES), F32)
    for item in range(2):
        first = item * 16 * depth + depth - shift_ref[item, 1]

        def fill(t, power, item=item, first=first):
            for k in range(8):
                rows = v_ref[pl.ds(first + t * 8 + k, 8, stride=2 * depth), :]
                u_ref[t, k, item] = rows
                power = power + rows * rows
            return power

        power = lax.fori_loop(0, slabs, fill, power)
    power_out[0:1] = jnp.sum(power, axis=0, keepdims=True)
    pl.semaphore_wait(barrier, slabs - 1 + GROUP - 1 + copies - 1)

    powers = exchange(
        slabs, slab, at_slab, lambda k: power_out.at[0:1], lambda k: power_in.at[k, 0:1], s_power, r_power)
    block = exchange(slabs, slab, at_slab, lambda k: blocks.at[k], lambda k: block_in.at[k], s_block, r_block)
    tilt = exchange(GROUP, g, at_group, lambda k: tilt_out.at[0:2], lambda k: tilt_in.at[k, 0:2], s_tilt, r_tilt)
    tilts = exchange(copies, r, at_copy, lambda k: tilts_out, lambda k: tilts_in.at[k], s_tilts, r_tilts)
    own = exchange(copies, r, at_copy, lambda k: own_out, lambda k: own_in.at[k], s_own, r_own)
    piece = exchange(
        slabs, slab, at_slab, lambda k: plane.at[pl.ds(pl.multiple_of(k * 8, 8), 8)], lambda k: pieces_in.at[k], s_piece, r_piece)
    whole = exchange(GROUP, g, at_group, lambda k: pieces_in, lambda k: planes_in.at[k], s_plane, r_plane)

    def rows(c):
        first, number = lax.rem(x + 1 + c, XS) * 2, 2
        if c >= XS - 1:
            first, number = x * 2 + (1 - p if c == XS - 1 else p), 1
        return first, number, exchange(
            slabs, slab, at_slab, lambda k: u_ref.at[k, pl.ds(first, number)],
            lambda k: rows_in.at[pl.ds(first, number), :, k], s_rows.at[c], r_rows.at[c], False)

    def part_copy(k):
        return pltpu.make_async_remote_copy(
            src_ref=part.at[k], dst_ref=parts_in.at[g], send_sem=s_part.at[k], recv_sem=r_part.at[g],
            device_id=at_group(k), device_id_type=MESH)

    def part_wait(k):
        return pltpu.make_async_remote_copy(
            src_ref=part.at[k], dst_ref=parts_in.at[k], send_sem=s_part.at[k], recv_sem=r_part.at[k],
            device_id=at_group(k), device_id_type=MESH)

    def whole_wait(k):
        pltpu.make_async_remote_copy(
            src_ref=pieces_in, dst_ref=planes_in.at[k], send_sem=s_plane.at[k], recv_sem=r_plane.at[k],
            device_id=at_group(k), device_id_type=MESH).wait_recv()

    def sums_over(turn):
        return exchange(
            GROUP, g, at_group, lambda k: some_out.at[turn, 0:1], lambda k: some_in.at[turn, k, 0:1], s_some.at[turn], r_some.at[turn],
        ), exchange(
            slabs, slab, at_slab, lambda k: more_out.at[turn, 0:1], lambda k: more_in.at[turn, k, 0:1], s_more.at[turn], r_more.at[turn])

    powers[0]()
    for c in range(CHUNKS):
        rows(c)[2][0]()
    loads[0].wait()

    def cut(t, carry):
        blocks[t] = s_ref[pl.ds(t * 8 + g, 8, stride=depth), :]
        return carry

    lax.fori_loop(0, slabs, cut, 0)
    block[0]()
    block_in[slab] = blocks[slab]
    power_in[slab, 0:1] = power_out[0:1]
    for k in range(8):
        for item in range(2):
            rows_in[k, item, slab] = u_ref[slab, k, item]

    lane = lax.broadcasted_iota(jnp.int32, (half, LANES), 1)
    row = lax.broadcasted_iota(jnp.int32, (half, LANES), 0)
    here = lane % HALF == row
    left = lane < HALF
    tile_row = lax.broadcasted_iota(jnp.int32, (8, LANES), 0)
    wide = lax.broadcasted_iota(jnp.int32, (tall, LANES), 1)

    spot = lax.broadcasted_iota(jnp.int32, (8, LANES), 1)
    edge = jnp.where(spot == 0, low_ref[0].astype(F32), jnp.where(spot == 1, low_ref[1].astype(F32), 0.0))
    edge = jnp.where(spot == 2, -high_ref[0].astype(F32), jnp.where(spot == 3, -high_ref[1].astype(F32), edge))
    edge = jnp.exp(edge * (1 / SOFTNESS))
    loads[1].wait()

    def table(k):
        return single[k * tall : (k + 1) * tall]

    def weight(p_table, q_table, low, high):
        return 1.0 / ((1.0 + p_table * high) * (1.0 + q_table * low))

    for item in range(2):
        low, high = edge[0:1, item : item + 1], edge[0:1, item + 2 : item + 3]
        w = weight(table(0), table(1), low, high)
        dw = weight(table(2), table(3), low, high) - w
        pick = wide == shift_ref[item, 0]
        zc = jnp.sum(jnp.where(pick, table(4), 0.0), axis=1, keepdims=True)
        zs = jnp.sum(jnp.where(pick, table(5), 0.0), axis=1, keepdims=True)
        first = 6 * tall + depth + 8
        xc = single[pl.ds(first + shift_ref[item, 2], 1), :]
        xs = single[pl.ds(first + LANES + shift_ref[item, 2], 1), :]
        cosine, sine = zc * xc - zs * xs, zs * xc + zc * xs
        factors[item, 0], factors[item, 1] = w * cosine, w * sine
        factors[item, 2], factors[item, 3] = dw * cosine, dw * sine

    powers[1]()
    energy = power_in[0, 0:1]
    for k in range(1, slabs):
        energy = energy + power_in[k, 0:1]
    tilt_out[0:1] = edge[0:1]
    tilt_out[1:2] = energy
    tilt[0]()
    tilt_in[g, 0:2] = tilt_out[0:2]
    for load in loads[2:]:
        load.wait()
    down, across, up = down_ref[...], across_ref[...], up_ref[...]

    def chunk(c):
        first, number, moved = rows(c)
        moved[1]()
        stack = []
        for k in range(number):
            for item in range(2):
                stack.append(table_by(down, rows_in[first + k, item].reshape(depth, LANES)))
        product = by_table(jnp.concatenate(stack, 0), across)
        for k in range(number):
            re = im = re_last = im_last = d_re = d_im = 0.0
            for item in range(2):
                at = (k * 2 + item) * (depth + 8)
                c_top, c_low, c_last = (product[at + a : at + b, :LANES] for a, b in ((0, half), (half, depth), (depth, depth + 8)))
                s_top, s_low, s_last = (product[at + a : at + b, LANES:] for a, b in ((0, half), (half, depth), (depth, depth + 8)))
                a, b = c_top + s_low, c_low - s_top
                wc, ws = factors[item, 0, :half], factors[item, 1, :half]
                re, im = re + wc * a + ws * b, im + wc * b - ws * a
                wc, ws = factors[item, 2, :half], factors[item, 3, :half]
                d_re, d_im = d_re + wc * a + ws * b, d_im + wc * b - ws * a
                wc, ws = factors[item, 0, half:], factors[item, 1, half:]
                re_last, im_last = re_last + wc * c_last - ws * s_last, im_last - wc * s_last - ws * c_last

            def lying(d):
                column = jnp.where(left, d[:, 0:1], d[:, HALF : HALF + 1])
                return jnp.sum(jnp.where(here, column, 0.0), axis=0, keepdims=True)

            last = jnp.where(tile_row == 0, re_last[0:1], jnp.where(tile_row == 1, im_last[0:1], 0.0))
            last = jnp.where(tile_row == 2, lying(d_re), jnp.where(tile_row == 3, lying(d_im), last))
            part[first + k, 0:half], part[first + k, half:depth] = re, im
            part[first + k, depth:] = last
        return first

    def add_up(ref, count):
        total = ref[0]
        for k in range(1, count):
            total = total + ref[k]
        return total

    for c in range(CHUNKS):
        first = chunk(c)
        if c < XS - 1:
            part_copy(first + 1 - p).start()
            part_copy(first + p).start()
        elif c == XS - 1:
            part_copy(first).start()
        if c == 0:
            tilt[1]()
            tilts_out[0:8] = jnp.concatenate([tilt_in[k, 0:1] for k in range(GROUP)], 0)
            energy = tilt_in[0, 1:2]
            for k in range(1, GROUP):
                energy = energy + tilt_in[k, 1:2]
            tilts_out[8:16] = jnp.broadcast_to(energy, (8, LANES))
            tilts[0]()
            tilts_in[r] = tilts_out[...]
        if c == 2:
            tilts[1]()
            energy = tilts_in[0, 8:9]
            for k in range(1, copies):
                energy = energy + tilts_in[k, 8:9]

            def square(k, totals):
                total, mirrored = totals
                for j in range(GROUP):
                    for item in range(2):
                        low, high = tilts_in[k, j : j + 1, item : item + 1], tilts_in[k, j : j + 1, item + 2 : item + 3]
                        w = weight(table(0), table(1), low, high)
                        total = total + w * w
                        w = weight(table(2), table(3), low, high)
                        mirrored = mirrored + w * w
                return total, mirrored

            none = jnp.zeros((tall, LANES), F32)
            total, mirrored = lax.fori_loop(0, copies, square, (none, none))

    parts_in[g] = part[g]
    each(GROUP, g, lambda k: part_wait(k).wait_recv())
    own_out[...] = add_up(parts_in, GROUP)
    own[0]()
    own_in[r] = own_out[...]

    def stacked(d):
        return jnp.concatenate([d[:half], d[:half], jnp.where(tile_row < 2, d[half : half + 1], 0.0)], 0)

    d_one, d_two = stacked(total), stacked(mirrored)
    block[1]()
    support = block_in[...].reshape(depth, LANES)
    sign = jnp.where(lax.broadcasted_iota(jnp.int32, (depth, LANES), 0) % 2 == 0, 1.0, -1.0) * (1 / math.sqrt(depth))
    count = single[6 * tall : 6 * tall + depth + 8]
    powers[2](), block[2](), tilt[2](), tilts[2]()
    for c in range(CHUNKS):
        rows(c)[2][2]()
    own[1]()
    sums = add_up(own_in, copies)

    def standing(values):
        spread = jnp.where(here, values, 0.0)
        one = jnp.sum(jnp.where(left, spread, 0.0), axis=1, keepdims=True)
        two = jnp.sum(jnp.where(left, 0.0, spread), axis=1, keepdims=True)
        return jnp.where(lane == 0, one, jnp.where(lane == HALF, two, 0.0))

    change = jnp.concatenate(
        [standing(sums[depth + 2 : depth + 3]), standing(sums[depth + 3 : depth + 4]), jnp.zeros((8, LANES), F32)], 0)
    sums = jnp.concatenate([sums[:depth], jnp.where(tile_row < 2, sums[depth:], 0.0)], 0)
    mean = jnp.zeros((depth + 8, LANES), F32)
    power = jnp.sum(energy, axis=(0, 1), keepdims=True)
    misfit = power * (1.0 / (subs * cells))
    mis_ref[0] = jnp.sum(misfit)
    for turn in range(ITERS):
        damping = REG_WEIGHT * subs * misfit + FLOOR_VALUE
        one, two = 0.5 / (d_one + damping), 0.5 / (d_two + damping)
        update = mean - mean * (d_one * one + d_two * two) + (one + two) * sums + two * change
        product = by_table(update, across)
        re = product[:half, :LANES] - product[half:depth, LANES:]
        im = product[half:depth, :LANES] + product[:half, LANES:]
        last = product[depth : depth + 1, :LANES] - product[depth + 1 : depth + 2, LANES:]
        field = table_by(up, jnp.concatenate([re, im], 0)) + sign * last
        if turn + 1 == ITERS:
            break
        product = by_table(table_by(down, support * field), across)
        last = jnp.where(tile_row == 0, product[depth : depth + 1, :LANES], -product[depth : depth + 1, LANES:])
        mean = jnp.concatenate([
            product[:half, :LANES] + product[half:depth, LANES:],
            product[half:depth, :LANES] - product[:half, LANES:],
            jnp.where(tile_row < 2, last, 0.0)], 0)
        terms = count * mean * (0.5 * (d_one + d_two) * mean - 2.0 * sums - change)
        some_out[turn, 0:1] = jnp.sum(terms, axis=0, keepdims=True)
        some, more = sums_over(turn)
        some[0]()
        some_in[turn, g, 0:1] = some_out[turn, 0:1]
        if turn == 0:
            own[2]()
            each(GROUP, g, lambda k: part_wait(k).wait_send(), False)
        some[1]()
        more_out[turn, 0:1] = add_up(some_in.at[turn, :, 0:1], GROUP)
        more[0]()
        more_in[turn, slab, 0:1] = more_out[turn, 0:1]
        more[1]()
        misfit = (power + jnp.sum(add_up(more_in.at[turn, :, 0:1], slabs), axis=(0, 1), keepdims=True)) * (1.0 / (subs * cells))
        mis_ref[turn + 1] = jnp.sum(misfit)
    plane[...] = field
    piece[0]()
    pieces_in[slab] = plane[pl.ds(pl.multiple_of(slab * 8, 8), 8)]

    piece[1]()
    whole[0]()

    def place(k, source):
        for j in range(slabs):
            out_ref[pl.ds(j * 8 + k, 8, stride=depth), :] = source[j]

    place(g, pieces_in)
    for turn in range(ITERS - 1):
        sums_over(turn)[0][2](), sums_over(turn)[1][2]()
    piece[2]()

    def arrived(k):
        whole_wait(k)
        place(k, planes_in.at[k])

    each(GROUP, g, arrived)
    whole[2]()


def body(volumes, tilt_low, tilt_high, shifts, support):
    slabs, ring = lax.axis_size("slab"), lax.axis_size("batch") // XS
    layer, ys, width = support.shape
    depth, copies, tall = layer * slabs, ring // 2, slabs * 8 + 8
    vmem, smem, hbm = (pl.BlockSpec(memory_space=space) for space in (pltpu.VMEM, pltpu.SMEM, pl.ANY))
    down, across, up, single = (jnp.asarray(table) for table in tables(depth, width))
    dma = pltpu.SemaphoreType.DMA

    def buffer(*shape):
        return pltpu.VMEM((*shape, LANES), F32)

    field, misfits = pl.pallas_call(
        functools.partial(refine, slabs, ring),
        out_shape=(jax.ShapeDtypeStruct((layer * ys, width), F32), jax.ShapeDtypeStruct((ITERS,), F32)),
        in_specs=[hbm] * 6 + [smem] * 3,
        out_specs=(vmem, smem),
        scratch_shapes=[
            buffer(2 * layer * 2 * ys), buffer(layer * ys), pltpu.VMEM(down.shape, BF16), pltpu.VMEM(across.shape, BF16),
            pltpu.VMEM(up.shape, BF16), buffer(single.shape[0]), buffer(slabs, 8, 2, 8), buffer(slabs, 8),
            buffer(8), buffer(slabs, 8), buffer(slabs, 8), buffer(8), buffer(GROUP, 8), buffer(16), buffer(copies, 16),
            buffer(8, 2, slabs, 8), buffer(2, 4, depth // 2 + 8),
            buffer(GROUP, tall), buffer(GROUP, tall), buffer(tall), buffer(copies, tall),
            buffer(2, 8), buffer(2, GROUP, 8), buffer(2, 8), buffer(2, slabs, 8),
            buffer(depth), buffer(slabs, 8), buffer(GROUP, slabs, 8), dma((5,)), dma((2, 16)),
            dma((slabs,)), dma((slabs,)), dma((slabs,)), dma((slabs,)), dma((GROUP,)), dma((GROUP,)), dma((copies,)), dma((copies,)),
            dma((CHUNKS, slabs)), dma((CHUNKS, slabs)), dma((GROUP,)), dma((GROUP,)), dma((copies,)), dma((copies,)),
            dma((2, GROUP)), dma((2, GROUP)), dma((2, slabs)), dma((2, slabs)),
            dma((slabs,)), dma((slabs,)), dma((GROUP,)), dma((GROUP,)),
        ],
        compiler_params=pltpu.CompilerParams(collective_id=0, has_side_effects=True),
        name="refine",
    )(volumes.reshape(2 * layer, ys, width), support.reshape(layer * ys, width), down, across, up, single, tilt_low, tilt_high, shifts)
    return support * field.reshape(layer, ys, width), misfits


def solution(mesh):
    placed = (
        P("batch", "slab", None, None),
        P("batch"),
        P("batch"),
        P("batch", None),
        P("slab", None, None),
    )
    return jax.shard_map(
        body, mesh=mesh, in_specs=placed, out_specs=(P("slab", None, None), P()), check_vma=False
    )
```

```python
import functools
import math

import jax
import jax.numpy as jnp
import numpy as np
from jax import lax
from jax.experimental import pallas as pl
from jax.experimental.pallas import tpu as pltpu
from jax.sharding import PartitionSpec as P

ITERS = 3
REG_WEIGHT = 0.5
FLOOR_VALUE = 1.0
SOFTNESS = 5.0
MESH = pl.DeviceIdType.MESH
LANES = 128
HALF = LANES // 2
XS = 4
GROUP = XS * 2
CHUNKS = 5
BATCHES = [(0, 3), (3, 5), (5, 8)]
F32 = jnp.float32
BF16 = jnp.bfloat16


def signed(length):
    index = np.arange(length)
    return np.where(index < length // 2, index, index - length)


def tables(depth, width):
    half = depth // 2
    kz, z = np.arange(half), np.arange(depth)
    angle = 2 * np.pi * (kz[:, None] * z[None, :] % depth) / depth
    scale = 1 / math.sqrt(depth)
    down = np.zeros((depth + 8, depth))
    down[:half], down[half:depth] = np.cos(angle) * scale, -np.sin(angle) * scale
    down[depth] = np.where(z % 2 == 0, 1, -1) * scale
    twice = np.where(kz == 0, 1, 2)[None, :]
    up = np.concatenate([np.cos(angle.T) * twice, -np.sin(angle.T) * twice], 1) * scale
    kx = np.arange(width)
    turn = 2 * np.pi * (kx[:, None] * kx[None, :] % width) / width
    across = np.concatenate([np.cos(turn), np.sin(turn)], 1) / math.sqrt(width)
    fz, fx = signed(depth), signed(width)
    theta = np.degrees(np.arctan2(fz[:, None] * np.where(fx >= 0, 1, -1)[None, :], np.abs(fx)[None, :] * 1.0))
    mirror = theta[(-z) % depth][:, (-kx) % width]
    rows = np.minimum(np.arange(half + 8), half)
    theta, mirror = theta[rows], mirror[rows]
    mirror[0], mirror[half:] = theta[0], theta[half:]
    shift = 2 * np.pi * (rows[:, None] * np.arange(LANES)[None, :] % depth) / depth
    wedge = [np.exp(theta / SOFTNESS), np.exp(-theta / SOFTNESS), np.exp(mirror / SOFTNESS), np.exp(-mirror / SOFTNESS)]
    count = np.zeros((depth + 8, LANES))
    count[:depth], count[depth : depth + 2] = 2, 1
    count[0] = count[half] = 1
    single = np.concatenate(wedge + [np.cos(shift), np.sin(shift), count, np.cos(turn), np.sin(turn)], 0)
    return split(down, 1), split(across, 0), split(up, 1), single.astype(np.float32)


def split(table, axis):
    table = table.astype(np.float32)
    high = table.astype(BF16)
    low = (table - high.astype(np.float32)).astype(BF16)
    return np.concatenate([high, high, low], axis)


def thirds(value, axis):
    high = value.astype(BF16)
    low = (value - high.astype(F32)).astype(BF16)
    return jnp.concatenate([high, low, high], axis)


def by_table(value, table):
    return jnp.dot(thirds(value, 1), table, preferred_element_type=F32)


def table_by(table, value):
    return jnp.dot(table, thirds(value, 0), preferred_element_type=F32)


def refine(
    slabs, ring, v_hbm, s_hbm, down_hbm, across_hbm, up_hbm, single_hbm, low_hbm, high_hbm, shift_hbm, out_ref, mis_ref,
    low_ref, high_ref, shift_ref,
    v_ref, s_ref, down_ref, across_ref, up_ref, single, u_ref, blocks,
    power_out, power_in, block_in, tilt_out, tilt_in, tilts_out, tilts_in, rows_in, factors, part, parts_in, own_out, own_in,
    some_out, some_in, more_out, more_in, plane, pieces_in, planes_in, s_load, s_volume,
    s_power, r_power, s_block, r_block, s_tilt, r_tilt, s_tilts, r_tilts, s_rows, r_rows, s_part, r_part, s_own, r_own,
    s_some, r_some, s_more, r_more, s_piece, r_piece, s_plane, r_plane,
):
    depth = slabs * 8
    half = depth // 2
    tall = half + 8
    copies = ring // 2
    subs = float(GROUP * copies * 2)
    cells = float(depth * depth * LANES)
    batch, slab = lax.axis_index("batch"), lax.axis_index("slab")
    x, y = batch // ring, batch % ring
    r, p = y // 2, y % 2
    g = x * 2 + p

    def at_slab(t):
        return (batch, t)

    def at_group(k):
        return (lax.div(k, 2) * ring + r * 2 + lax.rem(k, 2), slab)

    def at_copy(k):
        return (x * ring + k * 2 + p, slab)

    def each(count, me, act, unroll=True):
        if unroll:
            for off in sorted(range(1, count), key=lambda off: abs(off - count / 2)):
                act(lax.rem(me + off, count))
            return

        def step(k, carry):
            act(lax.rem(me + 1 + lax.rem(k + count // 4, count - 1), count))
            return carry

        if count > 1:
            lax.fori_loop(0, count - 1, step, 0)

    def exchange(count, me, device, source, target, send, recv, unroll=True):
        def copy(k, slot):
            return pltpu.make_async_remote_copy(
                src_ref=source(k), dst_ref=target(slot), send_sem=send.at[k], recv_sem=recv.at[slot],
                device_id=device(k), device_id_type=MESH,
            )

        return (
            lambda: each(count, me, lambda k: copy(k, me).start(), unroll),
            lambda: each(count, me, lambda k: copy(k, k).wait_recv(), unroll),
            lambda: each(count, me, lambda k: copy(k, me).wait_send(), False),
        )

    barrier = pltpu.get_barrier_semaphore()
    for count, me, device in ((slabs, slab, at_slab), (GROUP, g, at_group), (copies, r, at_copy)):
        each(count, me, lambda k, device=device: pl.semaphore_signal(
            barrier, inc=1, device_id=device(k), device_id_type=MESH))
    def volume_copy(k, again):
        return pltpu.make_async_copy(
            v_hbm.at[k], v_ref.at[pl.ds(pl.multiple_of(2 * depth * k + depth * again, depth), depth)], s_volume.at[again, k])

    loads = [
        pltpu.make_async_copy(source, target, s_load.at[k])
        for k, (source, target) in enumerate((
            (s_hbm, s_ref), (single_hbm, single), (down_hbm, down_ref), (across_hbm, across_ref), (up_hbm, up_ref),
            (low_hbm, low_ref), (high_hbm, high_ref), (shift_hbm, shift_ref)))
    ]

    def over(count, act):
        def step(k, carry):
            act(k)
            return carry

        lax.fori_loop(0, count, step, 0)

    for load in loads[5:]:
        load.start()
    for again in range(2):
        over(16, lambda k, again=again: volume_copy(k, again).start())
    for load in loads[:5]:
        load.start()
    for load in loads[5:]:
        load.wait()
    for again in range(2):
        over(16, lambda k, again=again: volume_copy(k, again).wait())
    power = jnp.zeros((8, LANES), F32)
    for item in range(2):
        first = item * 16 * depth + depth - shift_ref[item, 1]

        def fill(t, power, item=item, first=first):
            for k in range(8):
                rows = v_ref[pl.ds(first + t * 8 + k, 8, stride=2 * depth), :]
                u_ref[t, k, item] = rows
                power = power + rows * rows
            return power

        power = lax.fori_loop(0, slabs, fill, power)
    power_out[0:1] = jnp.sum(power, axis=0, keepdims=True)
    pl.semaphore_wait(barrier, slabs - 1 + GROUP - 1 + copies - 1)

    powers = exchange(
        slabs, slab, at_slab, lambda k: power_out.at[0:1], lambda k: power_in.at[k, 0:1], s_power, r_power)
    block = exchange(slabs, slab, at_slab, lambda k: blocks.at[k], lambda k: block_in.at[k], s_block, r_block)
    tilt = exchange(GROUP, g, at_group, lambda k: tilt_out.at[0:2], lambda k: tilt_in.at[k, 0:2], s_tilt, r_tilt)
    tilts = exchange(copies, r, at_copy, lambda k: tilts_out, lambda k: tilts_in.at[k], s_tilts, r_tilts)
    own = exchange(copies, r, at_copy, lambda k: own_out, lambda k: own_in.at[k], s_own, r_own)
    chips, chip, core = slabs // 2, lax.div(slab, 2), lax.rem(slab, 2)
    around = sorted(range(chips), key=lambda d: min(d, chips - d))

    def piece(place, there):
        target = lax.rem(chip + around[place], chips) * 2 + there
        slot = around.index((chips - around[place]) % chips) * 2 + core
        return pltpu.make_async_remote_copy(
            src_ref=plane.at[pl.ds(pl.multiple_of(target * 8, 8), 8)], dst_ref=pieces_in.at[slot],
            send_sem=s_piece.at[place * 2 + there], recv_sem=r_piece.at[slot], device_id=at_slab(target), device_id_type=MESH)

    def pieces(act, places):
        for place in places:
            for there in ((1 - core,) if place == 0 else (0, 1)):
                act(place, there)

    def piece_wait(place, there):
        pltpu.make_async_remote_copy(
            src_ref=plane.at[0:8], dst_ref=pieces_in.at[place * 2 + there], send_sem=s_piece.at[place * 2 + there],
            recv_sem=r_piece.at[place * 2 + there], device_id=at_slab(slab), device_id_type=MESH).wait_recv()

    def whole_copy(batch_of, k, slot):
        cut = slice(batch_of[0] * 2, batch_of[1] * 2)
        at = batches.index(batch_of)
        return pltpu.make_async_remote_copy(
            src_ref=pieces_in.at[cut], dst_ref=planes_in.at[slot, cut], send_sem=s_plane.at[at, k], recv_sem=r_plane.at[at, slot],
            device_id=at_group(k), device_id_type=MESH)

    batches = [cut for cut in BATCHES if cut[1] <= chips] or [(0, chips)]

    def rows(c):
        first, number = lax.rem(x + 1 + c, XS) * 2, 2
        if c >= XS - 1:
            first, number = x * 2 + (1 - p if c == XS - 1 else p), 1
        return first, number, exchange(
            slabs, slab, at_slab, lambda k: u_ref.at[k, pl.ds(first, number)],
            lambda k: rows_in.at[pl.ds(first, number), :, k], s_rows.at[c], r_rows.at[c])

    def part_copy(k):
        return pltpu.make_async_remote_copy(
            src_ref=part.at[k], dst_ref=parts_in.at[g], send_sem=s_part.at[k], recv_sem=r_part.at[g],
            device_id=at_group(k), device_id_type=MESH)

    def part_wait(k):
        return pltpu.make_async_remote_copy(
            src_ref=part.at[k], dst_ref=parts_in.at[k], send_sem=s_part.at[k], recv_sem=r_part.at[k],
            device_id=at_group(k), device_id_type=MESH)

    def sums_over(turn):
        return exchange(
            GROUP, g, at_group, lambda k: some_out.at[turn, 0:1], lambda k: some_in.at[turn, k, 0:1], s_some.at[turn], r_some.at[turn],
        ), exchange(
            slabs, slab, at_slab, lambda k: more_out.at[turn, 0:1], lambda k: more_in.at[turn, k, 0:1], s_more.at[turn], r_more.at[turn])

    powers[0]()
    for c in range(CHUNKS):
        rows(c)[2][0]()
    loads[0].wait()

    def cut(t, carry):
        blocks[t] = s_ref[pl.ds(t * 8 + g, 8, stride=depth), :]
        return carry

    lax.fori_loop(0, slabs, cut, 0)
    block[0]()
    block_in[slab] = blocks[slab]
    power_in[slab, 0:1] = power_out[0:1]
    for k in range(8):
        for item in range(2):
            rows_in[k, item, slab] = u_ref[slab, k, item]

    lane = lax.broadcasted_iota(jnp.int32, (half, LANES), 1)
    row = lax.broadcasted_iota(jnp.int32, (half, LANES), 0)
    here = lane % HALF == row
    left = lane < HALF
    tile_row = lax.broadcasted_iota(jnp.int32, (8, LANES), 0)
    wide = lax.broadcasted_iota(jnp.int32, (tall, LANES), 1)

    spot = lax.broadcasted_iota(jnp.int32, (8, LANES), 1)
    edge = jnp.where(spot == 0, low_ref[0].astype(F32), jnp.where(spot == 1, low_ref[1].astype(F32), 0.0))
    edge = jnp.where(spot == 2, -high_ref[0].astype(F32), jnp.where(spot == 3, -high_ref[1].astype(F32), edge))
    edge = jnp.exp(edge * (1 / SOFTNESS))
    loads[1].wait()

    def table(k):
        return single[k * tall : (k + 1) * tall]

    def weight(p_table, q_table, low, high):
        return 1.0 / ((1.0 + p_table * high) * (1.0 + q_table * low))

    for item in range(2):
        low, high = edge[0:1, item : item + 1], edge[0:1, item + 2 : item + 3]
        w = weight(table(0), table(1), low, high)
        dw = weight(table(2), table(3), low, high) - w
        pick = wide == shift_ref[item, 0]
        zc = jnp.sum(jnp.where(pick, table(4), 0.0), axis=1, keepdims=True)
        zs = jnp.sum(jnp.where(pick, table(5), 0.0), axis=1, keepdims=True)
        first = 6 * tall + depth + 8
        xc = single[pl.ds(first + shift_ref[item, 2], 1), :]
        xs = single[pl.ds(first + LANES + shift_ref[item, 2], 1), :]
        cosine, sine = zc * xc - zs * xs, zs * xc + zc * xs
        factors[item, 0], factors[item, 1] = w * cosine, w * sine
        factors[item, 2], factors[item, 3] = dw * cosine, dw * sine

    powers[1]()
    energy = power_in[0, 0:1]
    for k in range(1, slabs):
        energy = energy + power_in[k, 0:1]
    tilt_out[0:1] = edge[0:1]
    tilt_out[1:2] = energy
    tilt[0]()
    tilt_in[g, 0:2] = tilt_out[0:2]
    for load in loads[2:5]:
        load.wait()
    down, across, up = down_ref[...], across_ref[...], up_ref[...]

    def chunk(c):
        first, number, moved = rows(c)
        moved[1]()
        stack = []
        for k in range(number):
            for item in range(2):
                stack.append(table_by(down, rows_in[first + k, item].reshape(depth, LANES)))
        product = by_table(jnp.concatenate(stack, 0), across)
        for k in range(number):
            re = im = re_last = im_last = d_re = d_im = 0.0
            for item in range(2):
                at = (k * 2 + item) * (depth + 8)
                c_top, c_low, c_last = (product[at + a : at + b, :LANES] for a, b in ((0, half), (half, depth), (depth, depth + 8)))
                s_top, s_low, s_last = (product[at + a : at + b, LANES:] for a, b in ((0, half), (half, depth), (depth, depth + 8)))
                a, b = c_top + s_low, c_low - s_top
                wc, ws = factors[item, 0, :half], factors[item, 1, :half]
                re, im = re + wc * a + ws * b, im + wc * b - ws * a
                wc, ws = factors[item, 2, :half], factors[item, 3, :half]
                d_re, d_im = d_re + wc * a + ws * b, d_im + wc * b - ws * a
                wc, ws = factors[item, 0, half:], factors[item, 1, half:]
                re_last, im_last = re_last + wc * c_last - ws * s_last, im_last - wc * s_last - ws * c_last

            def lying(d):
                column = jnp.where(left, d[:, 0:1], d[:, HALF : HALF + 1])
                return jnp.sum(jnp.where(here, column, 0.0), axis=0, keepdims=True)

            last = jnp.where(tile_row == 0, re_last[0:1], jnp.where(tile_row == 1, im_last[0:1], 0.0))
            last = jnp.where(tile_row == 2, lying(d_re), jnp.where(tile_row == 3, lying(d_im), last))
            part[first + k, 0:half], part[first + k, half:depth] = re, im
            part[first + k, depth:] = last
        return first

    def add_up(ref, count):
        total = ref[0]
        for k in range(1, count):
            total = total + ref[k]
        return total

    for c in range(CHUNKS):
        first = chunk(c)
        if c < XS - 1:
            part_copy(first + 1 - p).start()
            part_copy(first + p).start()
        elif c == XS - 1:
            part_copy(first).start()
        if c == 0:
            tilt[1]()
            tilts_out[0:8] = jnp.concatenate([tilt_in[k, 0:1] for k in range(GROUP)], 0)
            energy = tilt_in[0, 1:2]
            for k in range(1, GROUP):
                energy = energy + tilt_in[k, 1:2]
            tilts_out[8:16] = jnp.broadcast_to(energy, (8, LANES))
            tilts[0]()
            tilts_in[r] = tilts_out[...]
        if c == 2:
            tilts[1]()
            energy = tilts_in[0, 8:9]
            for k in range(1, copies):
                energy = energy + tilts_in[k, 8:9]

            def square(k, totals):
                total, mirrored = totals
                for j in range(GROUP):
                    for item in range(2):
                        low, high = tilts_in[k, j : j + 1, item : item + 1], tilts_in[k, j : j + 1, item + 2 : item + 3]
                        w = weight(table(0), table(1), low, high)
                        total = total + w * w
                        w = weight(table(2), table(3), low, high)
                        mirrored = mirrored + w * w
                return total, mirrored

            none = jnp.zeros((tall, LANES), F32)
            total, mirrored = lax.fori_loop(0, copies, square, (none, none))

    parts_in[g] = part[g]
    each(GROUP, g, lambda k: part_wait(k).wait_recv())
    own_out[...] = add_up(parts_in, GROUP)
    own[0]()
    own_in[r] = own_out[...]

    def stacked(d):
        return jnp.concatenate([d[:half], d[:half], jnp.where(tile_row < 2, d[half : half + 1], 0.0)], 0)

    d_one, d_two = stacked(total), stacked(mirrored)
    block[1]()
    support = block_in[...].reshape(depth, LANES)
    sign = jnp.where(lax.broadcasted_iota(jnp.int32, (depth, LANES), 0) % 2 == 0, 1.0, -1.0) * (1 / math.sqrt(depth))
    count = single[6 * tall : 6 * tall + depth + 8]
    powers[2](), block[2](), tilt[2](), tilts[2]()
    for c in range(CHUNKS):
        rows(c)[2][2]()
    own[1]()
    sums = add_up(own_in, copies)

    def standing(values):
        spread = jnp.where(here, values, 0.0)
        one = jnp.sum(jnp.where(left, spread, 0.0), axis=1, keepdims=True)
        two = jnp.sum(jnp.where(left, 0.0, spread), axis=1, keepdims=True)
        return jnp.where(lane == 0, one, jnp.where(lane == HALF, two, 0.0))

    change = jnp.concatenate(
        [standing(sums[depth + 2 : depth + 3]), standing(sums[depth + 3 : depth + 4]), jnp.zeros((8, LANES), F32)], 0)
    sums = jnp.concatenate([sums[:depth], jnp.where(tile_row < 2, sums[depth:], 0.0)], 0)
    mean = jnp.zeros((depth + 8, LANES), F32)
    power = jnp.sum(energy, axis=(0, 1), keepdims=True)
    misfit = power * (1.0 / (subs * cells))
    mis_ref[0] = jnp.sum(misfit)
    for turn in range(ITERS):
        damping = REG_WEIGHT * subs * misfit + FLOOR_VALUE
        one, two = 0.5 / (d_one + damping), 0.5 / (d_two + damping)
        update = mean - mean * (d_one * one + d_two * two) + (one + two) * sums + two * change
        product = by_table(update, across)
        re = product[:half, :LANES] - product[half:depth, LANES:]
        im = product[half:depth, :LANES] + product[:half, LANES:]
        last = product[depth : depth + 1, :LANES] - product[depth + 1 : depth + 2, LANES:]
        field = table_by(up, jnp.concatenate([re, im], 0)) + sign * last
        if turn + 1 == ITERS:
            break
        product = by_table(table_by(down, support * field), across)
        last = jnp.where(tile_row == 0, product[depth : depth + 1, :LANES], -product[depth : depth + 1, LANES:])
        mean = jnp.concatenate([
            product[:half, :LANES] + product[half:depth, LANES:],
            product[half:depth, :LANES] - product[:half, LANES:],
            jnp.where(tile_row < 2, last, 0.0)], 0)
        terms = count * mean * (0.5 * (d_one + d_two) * mean - 2.0 * sums - change)
        some_out[turn, 0:1] = jnp.sum(terms, axis=0, keepdims=True)
        some, more = sums_over(turn)
        some[0]()
        some_in[turn, g, 0:1] = some_out[turn, 0:1]
        if turn == 0:
            own[2]()
            each(GROUP, g, lambda k: part_wait(k).wait_send(), False)
        some[1]()
        more_out[turn, 0:1] = add_up(some_in.at[turn, :, 0:1], GROUP)
        more[0]()
        more_in[turn, slab, 0:1] = more_out[turn, 0:1]
        more[1]()
        misfit = (power + jnp.sum(add_up(more_in.at[turn, :, 0:1], slabs), axis=(0, 1), keepdims=True)) * (1.0 / (subs * cells))
        mis_ref[turn + 1] = jnp.sum(misfit)
    plane[...] = field
    pieces(lambda place, there: piece(place, there).start(), range(chips))
    pieces_in[core] = plane[pl.ds(pl.multiple_of(slab * 8, 8), 8)]

    def place(k, source, cut):
        for at in range(*cut):
            for there in range(2):
                j = lax.rem(chip + around[at], chips) * 2 + there
                out_ref[pl.ds(j * 8 + k, 8, stride=depth), :] = source[at * 2 + there]

    for cut in batches:
        pieces(piece_wait, range(*cut))
        each(GROUP, g, lambda k: whole_copy(cut, k, g).start())
    for turn in range(ITERS - 1):
        sums_over(turn)[0][2](), sums_over(turn)[1][2]()
    pieces(lambda place, there: piece(place, there).wait_send(), range(chips))
    for cut in batches:
        place(g, pieces_in, cut)

        def arrived(k):
            whole_copy(cut, k, k).wait_recv()
            place(k, planes_in.at[k], cut)

        each(GROUP, g, arrived)
    for cut in batches:
        each(GROUP, g, lambda k: whole_copy(cut, k, g).wait_send())


def body(volumes, tilt_low, tilt_high, shifts, support):
    slabs, ring = lax.axis_size("slab"), lax.axis_size("batch") // XS
    layer, ys, width = support.shape
    depth, copies, tall = layer * slabs, ring // 2, slabs * 8 + 8
    vmem, smem, hbm = (pl.BlockSpec(memory_space=space) for space in (pltpu.VMEM, pltpu.SMEM, pl.ANY))
    down, across, up, single = (jnp.asarray(table) for table in tables(depth, width))
    dma = pltpu.SemaphoreType.DMA

    def buffer(*shape):
        return pltpu.VMEM((*shape, LANES), F32)

    field, misfits = pl.pallas_call(
        functools.partial(refine, slabs, ring),
        out_shape=(pltpu.VMEM((layer * ys, width), F32), jax.ShapeDtypeStruct((ITERS,), F32)),
        in_specs=[hbm] * 9,
        out_specs=(vmem, smem),
        scratch_shapes=[
            pltpu.SMEM((2,), jnp.int32), pltpu.SMEM((2,), jnp.int32), pltpu.SMEM((2, 3), jnp.int32),
            buffer(2 * layer * 2 * ys), buffer(layer * ys), pltpu.VMEM(down.shape, BF16), pltpu.VMEM(across.shape, BF16),
            pltpu.VMEM(up.shape, BF16), buffer(single.shape[0]), buffer(slabs, 8, 2, 8), buffer(slabs, 8),
            buffer(8), buffer(slabs, 8), buffer(slabs, 8), buffer(8), buffer(GROUP, 8), buffer(16), buffer(copies, 16),
            buffer(8, 2, slabs, 8), buffer(2, 4, depth // 2 + 8),
            buffer(GROUP, tall), buffer(GROUP, tall), buffer(tall), buffer(copies, tall),
            buffer(2, 8), buffer(2, GROUP, 8), buffer(2, 8), buffer(2, slabs, 8),
            buffer(depth), buffer(slabs, 8), buffer(GROUP, slabs, 8), dma((8,)), dma((2, 16)),
            dma((slabs,)), dma((slabs,)), dma((slabs,)), dma((slabs,)), dma((GROUP,)), dma((GROUP,)), dma((copies,)), dma((copies,)),
            dma((CHUNKS, slabs)), dma((CHUNKS, slabs)), dma((GROUP,)), dma((GROUP,)), dma((copies,)), dma((copies,)),
            dma((2, GROUP)), dma((2, GROUP)), dma((2, slabs)), dma((2, slabs)),
            dma((slabs,)), dma((slabs,)), dma((3, GROUP)), dma((3, GROUP)),
        ],
        compiler_params=pltpu.CompilerParams(collective_id=0, has_side_effects=True),
        name="refine",
    )(volumes.reshape(2 * layer, ys, width), support.reshape(layer * ys, width), down, across, up, single, tilt_low, tilt_high, shifts)
    return support * field.reshape(layer, ys, width), misfits


def solution(mesh):
    placed = (
        P("batch", "slab", None, None),
        P("batch"),
        P("batch"),
        P("batch", None),
        P("slab", None, None),
    )
    return jax.shard_map(
        body, mesh=mesh, in_specs=placed, out_specs=(P("slab", None, None), P()), check_vma=False
    )
```

```python
import functools
import math

import jax
import jax.numpy as jnp
import numpy as np
from jax import lax
from jax.experimental import pallas as pl
from jax.experimental.pallas import tpu as pltpu
from jax.sharding import PartitionSpec as P

ITERS = 3
REG_WEIGHT = 0.5
FLOOR_VALUE = 1.0
SOFTNESS = 5.0
MESH = pl.DeviceIdType.MESH
LANES = 128
HALF = LANES // 2
XS = 4
GROUP = XS * 2
CHUNKS = 5
BATCHES = [(0, 2), (2, 5), (5, 8)]
F32 = jnp.float32
BF16 = jnp.bfloat16


def signed(length):
    index = np.arange(length)
    return np.where(index < length // 2, index, index - length)


def tables(depth, width):
    half = depth // 2
    kz, z = np.arange(half), np.arange(depth)
    angle = 2 * np.pi * (kz[:, None] * z[None, :] % depth) / depth
    scale = 1 / math.sqrt(depth)
    down = np.zeros((depth + 8, depth))
    down[:half], down[half:depth] = np.cos(angle) * scale, -np.sin(angle) * scale
    down[depth] = np.where(z % 2 == 0, 1, -1) * scale
    twice = np.where(kz == 0, 1, 2)[None, :]
    up = np.concatenate([np.cos(angle.T) * twice, -np.sin(angle.T) * twice], 1) * scale
    kx = np.arange(width)
    turn = 2 * np.pi * (kx[:, None] * kx[None, :] % width) / width
    across = np.concatenate([np.cos(turn), np.sin(turn)], 1) / math.sqrt(width)
    fz, fx = signed(depth), signed(width)
    theta = np.degrees(np.arctan2(fz[:, None] * np.where(fx >= 0, 1, -1)[None, :], np.abs(fx)[None, :] * 1.0))
    mirror = theta[(-z) % depth][:, (-kx) % width]
    rows = np.minimum(np.arange(half + 8), half)
    theta, mirror = theta[rows], mirror[rows]
    mirror[0], mirror[half:] = theta[0], theta[half:]
    shift = 2 * np.pi * (rows[:, None] * np.arange(LANES)[None, :] % depth) / depth
    wedge = [np.exp(theta / SOFTNESS), np.exp(-theta / SOFTNESS), np.exp(mirror / SOFTNESS), np.exp(-mirror / SOFTNESS)]
    count = np.zeros((depth + 8, LANES))
    count[:depth], count[depth : depth + 2] = 2, 1
    count[0] = count[half] = 1
    single = np.concatenate(wedge + [np.cos(shift), np.sin(shift), count, np.cos(turn), np.sin(turn)], 0)
    return split(down, 1), split(across, 0), split(up, 1), single.astype(np.float32)


def split(table, axis):
    table = table.astype(np.float32)
    high = table.astype(BF16)
    low = (table - high.astype(np.float32)).astype(BF16)
    return np.concatenate([high, high, low], axis)


def thirds(value, axis):
    high = value.astype(BF16)
    low = (value - high.astype(F32)).astype(BF16)
    return jnp.concatenate([high, low, high], axis)


def by_table(value, table):
    return jnp.dot(thirds(value, 1), table, preferred_element_type=F32)


def table_by(table, value):
    return jnp.dot(table, thirds(value, 0), preferred_element_type=F32)


def refine(
    slabs, ring, v_hbm, s_hbm, down_hbm, across_hbm, up_hbm, single_hbm, low_hbm, high_hbm, shift_hbm, out_ref, mis_ref,
    low_ref, high_ref, shift_ref,
    v_ref, s_ref, down_ref, across_ref, up_ref, single, u_ref, blocks,
    power_out, power_in, block_in, tilt_out, tilt_in, tilts_out, tilts_in, rows_in, factors, part, parts_in, own_out, own_in,
    some_out, some_in, more_out, more_in, plane, pieces_in, planes_in, s_load, s_volume,
    s_power, r_power, s_block, r_block, s_tilt, r_tilt, s_tilts, r_tilts, s_rows, r_rows, s_part, r_part, s_own, r_own,
    s_some, r_some, s_more, r_more, s_piece, r_piece, s_plane, r_plane,
):
    depth = slabs * 8
    half = depth // 2
    tall = half + 8
    copies = ring // 2
    subs = float(GROUP * copies * 2)
    cells = float(depth * depth * LANES)
    batch, slab = lax.axis_index("batch"), lax.axis_index("slab")
    x, y = batch // ring, batch % ring
    r, p = y // 2, y % 2
    g = x * 2 + p

    def at_slab(t):
        return (batch, t)

    def at_group(k):
        return (lax.div(k, 2) * ring + r * 2 + lax.rem(k, 2), slab)

    def at_copy(k):
        return (x * ring + k * 2 + p, slab)

    def each(count, me, act, unroll=True):
        if unroll:
            for off in sorted(range(1, count), key=lambda off: abs(off - count / 2)):
                act(lax.rem(me + off, count))
            return

        def step(k, carry):
            act(lax.rem(me + 1 + lax.rem(k + count // 4, count - 1), count))
            return carry

        if count > 1:
            lax.fori_loop(0, count - 1, step, 0)

    def exchange(count, me, device, source, target, send, recv, unroll=True):
        def copy(k, slot):
            return pltpu.make_async_remote_copy(
                src_ref=source(k), dst_ref=target(slot), send_sem=send.at[k], recv_sem=recv.at[slot],
                device_id=device(k), device_id_type=MESH,
            )

        return (
            lambda: each(count, me, lambda k: copy(k, me).start(), unroll),
            lambda: each(count, me, lambda k: copy(k, k).wait_recv(), unroll),
            lambda: each(count, me, lambda k: copy(k, me).wait_send(), False),
        )

    barrier = pltpu.get_barrier_semaphore()
    for count, me, device in ((slabs, slab, at_slab), (GROUP, g, at_group), (copies, r, at_copy)):
        each(count, me, lambda k, device=device: pl.semaphore_signal(
            barrier, inc=1, device_id=device(k), device_id_type=MESH))
    def volume_copy(k, again):
        return pltpu.make_async_copy(
            v_hbm.at[k], v_ref.at[pl.ds(pl.multiple_of(2 * depth * k + depth * again, depth), depth)], s_volume.at[again, k])

    loads = [
        pltpu.make_async_copy(source, target, s_load.at[k])
        for k, (source, target) in enumerate((
            (s_hbm, s_ref), (single_hbm, single), (down_hbm, down_ref), (across_hbm, across_ref), (up_hbm, up_ref),
            (low_hbm, low_ref), (high_hbm, high_ref), (shift_hbm, shift_ref)))
    ]

    def over(count, act):
        def step(k, carry):
            act(k)
            return carry

        lax.fori_loop(0, count, step, 0)

    for load in loads[5:]:
        load.start()
    for again in range(2):
        over(16, lambda k, again=again: volume_copy(k, again).start())
    for load in loads[:5]:
        load.start()
    for load in loads[5:]:
        load.wait()
    for again in range(2):
        over(16, lambda k, again=again: volume_copy(k, again).wait())
    power = jnp.zeros((8, LANES), F32)
    for item in range(2):
        first = item * 16 * depth + depth - shift_ref[item, 1]

        def fill(t, power, item=item, first=first):
            for k in range(8):
                rows = v_ref[pl.ds(first + t * 8 + k, 8, stride=2 * depth), :]
                u_ref[t, k, item] = rows
                power = power + rows * rows
            return power

        power = lax.fori_loop(0, slabs, fill, power)
    power_out[0:1] = jnp.sum(power, axis=0, keepdims=True)
    pl.semaphore_wait(barrier, slabs - 1 + GROUP - 1 + copies - 1)

    powers = exchange(
        slabs, slab, at_slab, lambda k: power_out.at[0:1], lambda k: power_in.at[k, 0:1], s_power, r_power)
    block = exchange(slabs, slab, at_slab, lambda k: blocks.at[k], lambda k: block_in.at[k], s_block, r_block)
    tilt = exchange(GROUP, g, at_group, lambda k: tilt_out.at[0:2], lambda k: tilt_in.at[k, 0:2], s_tilt, r_tilt)
    tilts = exchange(copies, r, at_copy, lambda k: tilts_out, lambda k: tilts_in.at[k], s_tilts, r_tilts)
    own = exchange(copies, r, at_copy, lambda k: own_out, lambda k: own_in.at[k], s_own, r_own)
    chips, chip, core = slabs // 2, lax.div(slab, 2), lax.rem(slab, 2)
    around = sorted(range(chips), key=lambda d: min(d, chips - d))

    def piece(place, there):
        target = lax.rem(chip + around[place], chips) * 2 + there
        slot = around.index((chips - around[place]) % chips) * 2 + core
        return pltpu.make_async_remote_copy(
            src_ref=plane.at[pl.ds(pl.multiple_of(target * 8, 8), 8)], dst_ref=pieces_in.at[slot],
            send_sem=s_piece.at[place * 2 + there], recv_sem=r_piece.at[slot], device_id=at_slab(target), device_id_type=MESH)

    def pieces(act, places):
        for place in places:
            for there in ((1 - core,) if place == 0 else (0, 1)):
                act(place, there)

    def piece_wait(place, there):
        pltpu.make_async_remote_copy(
            src_ref=plane.at[0:8], dst_ref=pieces_in.at[place * 2 + there], send_sem=s_piece.at[place * 2 + there],
            recv_sem=r_piece.at[place * 2 + there], device_id=at_slab(slab), device_id_type=MESH).wait_recv()

    def whole_copy(batch_of, k, slot):
        cut = slice(batch_of[0] * 2, batch_of[1] * 2)
        at = batches.index(batch_of)
        return pltpu.make_async_remote_copy(
            src_ref=pieces_in.at[cut], dst_ref=planes_in.at[slot, cut], send_sem=s_plane.at[at, k], recv_sem=r_plane.at[at, slot],
            device_id=at_group(k), device_id_type=MESH)

    batches = [cut for cut in BATCHES if cut[1] <= chips] or [(0, chips)]

    def rows(c):
        first, number = lax.rem(x + 1 + c, XS) * 2, 2
        if c >= XS - 1:
            first, number = x * 2 + (1 - p if c == XS - 1 else p), 1
        return first, number, exchange(
            slabs, slab, at_slab, lambda k: u_ref.at[k, pl.ds(first, number)],
            lambda k: rows_in.at[pl.ds(first, number), :, k], s_rows.at[c], r_rows.at[c])

    def part_copy(k):
        return pltpu.make_async_remote_copy(
            src_ref=part.at[k], dst_ref=parts_in.at[g], send_sem=s_part.at[k], recv_sem=r_part.at[g],
            device_id=at_group(k), device_id_type=MESH)

    def part_wait(k):
        return pltpu.make_async_remote_copy(
            src_ref=part.at[k], dst_ref=parts_in.at[k], send_sem=s_part.at[k], recv_sem=r_part.at[k],
            device_id=at_group(k), device_id_type=MESH)

    def sums_over(turn):
        return exchange(
            GROUP, g, at_group, lambda k: some_out.at[turn, 0:1], lambda k: some_in.at[turn, k, 0:1], s_some.at[turn], r_some.at[turn],
        ), exchange(
            slabs, slab, at_slab, lambda k: more_out.at[turn, 0:1], lambda k: more_in.at[turn, k, 0:1], s_more.at[turn], r_more.at[turn])

    powers[0]()
    for c in range(CHUNKS):
        rows(c)[2][0]()
    loads[0].wait()

    def cut(t, carry):
        blocks[t] = s_ref[pl.ds(t * 8 + g, 8, stride=depth), :]
        return carry

    lax.fori_loop(0, slabs, cut, 0)
    block[0]()
    block_in[slab] = blocks[slab]
    power_in[slab, 0:1] = power_out[0:1]
    for k in range(8):
        for item in range(2):
            rows_in[k, item, slab] = u_ref[slab, k, item]

    lane = lax.broadcasted_iota(jnp.int32, (half, LANES), 1)
    row = lax.broadcasted_iota(jnp.int32, (half, LANES), 0)
    here = lane % HALF == row
    left = lane < HALF
    tile_row = lax.broadcasted_iota(jnp.int32, (8, LANES), 0)
    wide = lax.broadcasted_iota(jnp.int32, (tall, LANES), 1)

    spot = lax.broadcasted_iota(jnp.int32, (8, LANES), 1)
    edge = jnp.where(spot == 0, low_ref[0].astype(F32), jnp.where(spot == 1, low_ref[1].astype(F32), 0.0))
    edge = jnp.where(spot == 2, -high_ref[0].astype(F32), jnp.where(spot == 3, -high_ref[1].astype(F32), edge))
    edge = jnp.exp(edge * (1 / SOFTNESS))
    loads[1].wait()

    def table(k):
        return single[k * tall : (k + 1) * tall]

    def weight(p_table, q_table, low, high):
        return 1.0 / ((1.0 + p_table * high) * (1.0 + q_table * low))

    for item in range(2):
        low, high = edge[0:1, item : item + 1], edge[0:1, item + 2 : item + 3]
        w = weight(table(0), table(1), low, high)
        dw = weight(table(2), table(3), low, high) - w
        pick = wide == shift_ref[item, 0]
        zc = jnp.sum(jnp.where(pick, table(4), 0.0), axis=1, keepdims=True)
        zs = jnp.sum(jnp.where(pick, table(5), 0.0), axis=1, keepdims=True)
        first = 6 * tall + depth + 8
        xc = single[pl.ds(first + shift_ref[item, 2], 1), :]
        xs = single[pl.ds(first + LANES + shift_ref[item, 2], 1), :]
        cosine, sine = zc * xc - zs * xs, zs * xc + zc * xs
        factors[item, 0], factors[item, 1] = w * cosine, w * sine
        factors[item, 2], factors[item, 3] = dw * cosine, dw * sine

    powers[1]()
    energy = power_in[0, 0:1]
    for k in range(1, slabs):
        energy = energy + power_in[k, 0:1]
    tilt_out[0:1] = edge[0:1]
    tilt_out[1:2] = energy
    tilt[0]()
    tilt_in[g, 0:2] = tilt_out[0:2]
    for load in loads[2:5]:
        load.wait()
    down, across, up = down_ref[...], across_ref[...], up_ref[...]

    def chunk(c):
        first, number, moved = rows(c)
        moved[1]()
        stack = []
        for k in range(number):
            for item in range(2):
                stack.append(table_by(down, rows_in[first + k, item].reshape(depth, LANES)))
        product = by_table(jnp.concatenate(stack, 0), across)
        for k in range(number):
            re = im = re_last = im_last = d_re = d_im = 0.0
            for item in range(2):
                at = (k * 2 + item) * (depth + 8)
                c_top, c_low, c_last = (product[at + a : at + b, :LANES] for a, b in ((0, half), (half, depth), (depth, depth + 8)))
                s_top, s_low, s_last = (product[at + a : at + b, LANES:] for a, b in ((0, half), (half, depth), (depth, depth + 8)))
                a, b = c_top + s_low, c_low - s_top
                wc, ws = factors[item, 0, :half], factors[item, 1, :half]
                re, im = re + wc * a + ws * b, im + wc * b - ws * a
                wc, ws = factors[item, 2, :half], factors[item, 3, :half]
                d_re, d_im = d_re + wc * a + ws * b, d_im + wc * b - ws * a
                wc, ws = factors[item, 0, half:], factors[item, 1, half:]
                re_last, im_last = re_last + wc * c_last - ws * s_last, im_last - wc * s_last - ws * c_last

            def lying(d):
                column = jnp.where(left, d[:, 0:1], d[:, HALF : HALF + 1])
                return jnp.sum(jnp.where(here, column, 0.0), axis=0, keepdims=True)

            last = jnp.where(tile_row == 0, re_last[0:1], jnp.where(tile_row == 1, im_last[0:1], 0.0))
            last = jnp.where(tile_row == 2, lying(d_re), jnp.where(tile_row == 3, lying(d_im), last))
            part[first + k, 0:half], part[first + k, half:depth] = re, im
            part[first + k, depth:] = last
        return first

    def add_up(ref, count):
        total = ref[0]
        for k in range(1, count):
            total = total + ref[k]
        return total

    for c in range(CHUNKS):
        first = chunk(c)
        if c < XS - 1:
            part_copy(first + 1 - p).start()
            part_copy(first + p).start()
        elif c == XS - 1:
            part_copy(first).start()
        if c == 0:
            tilt[1]()
            tilts_out[0:8] = jnp.concatenate([tilt_in[k, 0:1] for k in range(GROUP)], 0)
            energy = tilt_in[0, 1:2]
            for k in range(1, GROUP):
                energy = energy + tilt_in[k, 1:2]
            tilts_out[8:16] = jnp.broadcast_to(energy, (8, LANES))
            tilts[0]()
            tilts_in[r] = tilts_out[...]
        if c == 2:
            tilts[1]()
            energy = tilts_in[0, 8:9]
            for k in range(1, copies):
                energy = energy + tilts_in[k, 8:9]

            def square(k, totals):
                total, mirrored = totals
                for j in range(GROUP):
                    for item in range(2):
                        low, high = tilts_in[k, j : j + 1, item : item + 1], tilts_in[k, j : j + 1, item + 2 : item + 3]
                        w = weight(table(0), table(1), low, high)
                        total = total + w * w
                        w = weight(table(2), table(3), low, high)
                        mirrored = mirrored + w * w
                return total, mirrored

            none = jnp.zeros((tall, LANES), F32)
            total, mirrored = lax.fori_loop(0, copies, square, (none, none))

    parts_in[g] = part[g]
    each(GROUP, g, lambda k: part_wait(k).wait_recv())
    own_out[...] = add_up(parts_in, GROUP)
    own[0]()
    own_in[r] = own_out[...]

    def stacked(d):
        return jnp.concatenate([d[:half], d[:half], jnp.where(tile_row < 2, d[half : half + 1], 0.0)], 0)

    d_one, d_two = stacked(total), stacked(mirrored)
    block[1]()
    support = block_in[...].reshape(depth, LANES)
    sign = jnp.where(lax.broadcasted_iota(jnp.int32, (depth, LANES), 0) % 2 == 0, 1.0, -1.0) * (1 / math.sqrt(depth))
    count = single[6 * tall : 6 * tall + depth + 8]
    powers[2](), block[2](), tilt[2](), tilts[2]()
    for c in range(CHUNKS):
        rows(c)[2][2]()
    own[1]()
    sums = add_up(own_in, copies)

    def standing(values):
        spread = jnp.where(here, values, 0.0)
        one = jnp.sum(jnp.where(left, spread, 0.0), axis=1, keepdims=True)
        two = jnp.sum(jnp.where(left, 0.0, spread), axis=1, keepdims=True)
        return jnp.where(lane == 0, one, jnp.where(lane == HALF, two, 0.0))

    change = jnp.concatenate(
        [standing(sums[depth + 2 : depth + 3]), standing(sums[depth + 3 : depth + 4]), jnp.zeros((8, LANES), F32)], 0)
    sums = jnp.concatenate([sums[:depth], jnp.where(tile_row < 2, sums[depth:], 0.0)], 0)
    mean = jnp.zeros((depth + 8, LANES), F32)
    power = jnp.sum(energy, axis=(0, 1), keepdims=True)
    misfit = power * (1.0 / (subs * cells))
    misfits = [misfit]
    for turn in range(ITERS):
        damping = REG_WEIGHT * subs * misfit + FLOOR_VALUE
        one, two = 0.5 / (d_one + damping), 0.5 / (d_two + damping)
        update = mean - mean * (d_one * one + d_two * two) + (one + two) * sums + two * change
        product = by_table(update, across)
        re = product[:half, :LANES] - product[half:depth, LANES:]
        im = product[half:depth, :LANES] + product[:half, LANES:]
        last = product[depth : depth + 1, :LANES] - product[depth + 1 : depth + 2, LANES:]
        field = table_by(up, jnp.concatenate([re, im], 0)) + sign * last
        if turn + 1 == ITERS:
            break
        product = by_table(table_by(down, support * field), across)
        last = jnp.where(tile_row == 0, product[depth : depth + 1, :LANES], -product[depth : depth + 1, LANES:])
        mean = jnp.concatenate([
            product[:half, :LANES] + product[half:depth, LANES:],
            product[half:depth, :LANES] - product[:half, LANES:],
            jnp.where(tile_row < 2, last, 0.0)], 0)
        terms = count * mean * (0.5 * (d_one + d_two) * mean - 2.0 * sums - change)
        some_out[turn, 0:1] = jnp.sum(terms, axis=0, keepdims=True)
        some, more = sums_over(turn)
        some[0]()
        some_in[turn, g, 0:1] = some_out[turn, 0:1]
        if turn == 0:
            own[2]()
            each(GROUP, g, lambda k: part_wait(k).wait_send(), False)
        some[1]()
        more_out[turn, 0:1] = add_up(some_in.at[turn, :, 0:1], GROUP)
        more[0]()
        more_in[turn, slab, 0:1] = more_out[turn, 0:1]
        more[1]()
        misfit = (power + jnp.sum(add_up(more_in.at[turn, :, 0:1], slabs), axis=(0, 1), keepdims=True)) * (1.0 / (subs * cells))
        misfits.append(misfit)
    plane[...] = field
    pieces(lambda place, there: piece(place, there).start(), range(chips))
    pieces_in[core] = plane[pl.ds(pl.multiple_of(slab * 8, 8), 8)]

    def place(k, source, cut):
        for at in range(*cut):
            for there in range(2):
                j = lax.rem(chip + around[at], chips) * 2 + there
                out_ref[pl.ds(j * 8 + k, 8, stride=depth), :] = source[at * 2 + there]

    for cut in batches:
        pieces(piece_wait, range(*cut))
        each(GROUP, g, lambda k: whole_copy(cut, k, g).start())
    for turn in range(ITERS):
        mis_ref[turn] = jnp.sum(misfits[turn])
    for turn in range(ITERS - 1):
        sums_over(turn)[0][2](), sums_over(turn)[1][2]()
    pieces(lambda place, there: piece(place, there).wait_send(), range(chips))
    for cut in batches:
        place(g, pieces_in, cut)

        def arrived(k):
            whole_copy(cut, k, k).wait_recv()
            place(k, planes_in.at[k], cut)

        each(GROUP, g, arrived)
    for cut in batches:
        each(GROUP, g, lambda k: whole_copy(cut, k, g).wait_send())


def body(volumes, tilt_low, tilt_high, shifts, support):
    slabs, ring = lax.axis_size("slab"), lax.axis_size("batch") // XS
    layer, ys, width = support.shape
    depth, copies, tall = layer * slabs, ring // 2, slabs * 8 + 8
    vmem, smem, hbm = (pl.BlockSpec(memory_space=space) for space in (pltpu.VMEM, pltpu.SMEM, pl.ANY))
    down, across, up, single = (jnp.asarray(table) for table in tables(depth, width))
    dma = pltpu.SemaphoreType.DMA

    def buffer(*shape):
        return pltpu.VMEM((*shape, LANES), F32)

    field, misfits = pl.pallas_call(
        functools.partial(refine, slabs, ring),
        out_shape=(pltpu.VMEM((layer * ys, width), F32), jax.ShapeDtypeStruct((ITERS,), F32)),
        in_specs=[hbm] * 9,
        out_specs=(vmem, smem),
        scratch_shapes=[
            pltpu.SMEM((2,), jnp.int32), pltpu.SMEM((2,), jnp.int32), pltpu.SMEM((2, 3), jnp.int32),
            buffer(2 * layer * 2 * ys), buffer(layer * ys), pltpu.VMEM(down.shape, BF16), pltpu.VMEM(across.shape, BF16),
            pltpu.VMEM(up.shape, BF16), buffer(single.shape[0]), buffer(slabs, 8, 2, 8), buffer(slabs, 8),
            buffer(8), buffer(slabs, 8), buffer(slabs, 8), buffer(8), buffer(GROUP, 8), buffer(16), buffer(copies, 16),
            buffer(8, 2, slabs, 8), buffer(2, 4, depth // 2 + 8),
            buffer(GROUP, tall), buffer(GROUP, tall), buffer(tall), buffer(copies, tall),
            buffer(2, 8), buffer(2, GROUP, 8), buffer(2, 8), buffer(2, slabs, 8),
            buffer(depth), buffer(slabs, 8), buffer(GROUP, slabs, 8), dma((8,)), dma((2, 16)),
            dma((slabs,)), dma((slabs,)), dma((slabs,)), dma((slabs,)), dma((GROUP,)), dma((GROUP,)), dma((copies,)), dma((copies,)),
            dma((CHUNKS, slabs)), dma((CHUNKS, slabs)), dma((GROUP,)), dma((GROUP,)), dma((copies,)), dma((copies,)),
            dma((2, GROUP)), dma((2, GROUP)), dma((2, slabs)), dma((2, slabs)),
            dma((slabs,)), dma((slabs,)), dma((3, GROUP)), dma((3, GROUP)),
        ],
        compiler_params=pltpu.CompilerParams(collective_id=0, has_side_effects=True),
        name="refine",
    )(volumes.reshape(2 * layer, ys, width), support.reshape(layer * ys, width), down, across, up, single, tilt_low, tilt_high, shifts)
    return support * field.reshape(layer, ys, width), misfits


def solution(mesh):
    placed = (
        P("batch", "slab", None, None),
        P("batch"),
        P("batch"),
        P("batch", None),
        P("slab", None, None),
    )
    return jax.shard_map(
        body, mesh=mesh, in_specs=placed, out_specs=(P("slab", None, None), P()), check_vma=False
    )
```

```python
import functools
import math

import jax
import jax.numpy as jnp
import numpy as np
from jax import lax
from jax.experimental import pallas as pl
from jax.experimental.pallas import tpu as pltpu
from jax.sharding import PartitionSpec as P

ITERS = 3
REG_WEIGHT = 0.5
FLOOR_VALUE = 1.0
SOFTNESS = 5.0
MESH = pl.DeviceIdType.MESH
LANES = 128
HALF = LANES // 2
XS = 4
GROUP = XS * 2
CHUNKS = 5
BATCHES = [(0, 2), (2, 5), (5, 8)]
F32 = jnp.float32
BF16 = jnp.bfloat16


def signed(length):
    index = np.arange(length)
    return np.where(index < length // 2, index, index - length)


def tables(depth, width):
    half = depth // 2
    kz, z = np.arange(half), np.arange(depth)
    angle = 2 * np.pi * (kz[:, None] * z[None, :] % depth) / depth
    scale = 1 / math.sqrt(depth)
    down = np.zeros((depth + 8, depth))
    down[:half], down[half:depth] = np.cos(angle) * scale, -np.sin(angle) * scale
    down[depth] = np.where(z % 2 == 0, 1, -1) * scale
    twice = np.where(kz == 0, 1, 2)[None, :]
    up = np.concatenate([np.cos(angle.T) * twice, -np.sin(angle.T) * twice], 1) * scale
    kx = np.arange(width)
    turn = 2 * np.pi * (kx[:, None] * kx[None, :] % width) / width
    across = np.concatenate([np.cos(turn), np.sin(turn)], 1) / math.sqrt(width)
    fz, fx = signed(depth), signed(width)
    theta = np.degrees(np.arctan2(fz[:, None] * np.where(fx >= 0, 1, -1)[None, :], np.abs(fx)[None, :] * 1.0))
    mirror = theta[(-z) % depth][:, (-kx) % width]
    rows = np.minimum(np.arange(half + 8), half)
    theta, mirror = theta[rows], mirror[rows]
    mirror[0], mirror[half:] = theta[0], theta[half:]
    shift = 2 * np.pi * (rows[:, None] * np.arange(LANES)[None, :] % depth) / depth
    wedge = [np.exp(theta / SOFTNESS), np.exp(-theta / SOFTNESS), np.exp(mirror / SOFTNESS), np.exp(-mirror / SOFTNESS)]
    count = np.zeros((depth + 8, LANES))
    count[:depth], count[depth : depth + 2] = 2, 1
    count[0] = count[half] = 1
    single = np.concatenate(wedge + [np.cos(shift), np.sin(shift), count, np.cos(turn), np.sin(turn)], 0)
    return split(down, 1), split(across, 0), split(up, 1), single.astype(np.float32)


def split(table, axis):
    table = table.astype(np.float32)
    high = table.astype(BF16)
    low = (table - high.astype(np.float32)).astype(BF16)
    return np.concatenate([high, high, low], axis)


def thirds(value, axis):
    high = value.astype(BF16)
    low = (value - high.astype(F32)).astype(BF16)
    return jnp.concatenate([high, low, high], axis)


def by_table(value, table):
    return jnp.dot(thirds(value, 1), table, preferred_element_type=F32)


def table_by(table, value):
    return jnp.dot(table, thirds(value, 0), preferred_element_type=F32)


def refine(
    slabs, ring, v_hbm, s_hbm, down_hbm, across_hbm, up_hbm, single_hbm, low_hbm, high_hbm, shift_hbm, out_ref, mis_ref,
    low_ref, high_ref, shift_ref,
    v_ref, s_ref, down_ref, across_ref, up_ref, single, u_ref, blocks,
    power_out, power_in, block_in, tilt_out, tilt_in, tilts_out, tilts_in, rows_in, factors, part, parts_in, own_out, own_in,
    some_out, some_in, more_out, more_in, plane, pieces_in, planes_in, s_load, s_volume,
    s_power, r_power, s_block, r_block, s_tilt, r_tilt, s_tilts, r_tilts, s_rows, r_rows, s_part, r_part, s_own, r_own,
    s_some, r_some, s_more, r_more, s_piece, r_piece, s_plane, r_plane,
):
    depth = slabs * 8
    half = depth // 2
    tall = half + 8
    copies = ring // 2
    subs = float(GROUP * copies * 2)
    cells = float(depth * depth * LANES)
    batch, slab = lax.axis_index("batch"), lax.axis_index("slab")
    x, y = batch // ring, batch % ring
    r, p = y // 2, y % 2
    g = x * 2 + p

    def at_slab(t):
        return (batch, t)

    def at_group(k):
        return (lax.div(k, 2) * ring + r * 2 + lax.rem(k, 2), slab)

    def at_copy(k):
        return (x * ring + k * 2 + p, slab)

    def each(count, me, act, unroll=True):
        if unroll:
            for off in sorted(range(1, count), key=lambda off: abs(off - count / 2)):
                act(lax.rem(me + off, count))
            return

        def step(k, carry):
            act(lax.rem(me + 1 + lax.rem(k + count // 4, count - 1), count))
            return carry

        if count > 1:
            lax.fori_loop(0, count - 1, step, 0)

    def exchange(count, me, device, source, target, send, recv, unroll=True):
        def copy(k, slot):
            return pltpu.make_async_remote_copy(
                src_ref=source(k), dst_ref=target(slot), send_sem=send.at[k], recv_sem=recv.at[slot],
                device_id=device(k), device_id_type=MESH,
            )

        return (
            lambda: each(count, me, lambda k: copy(k, me).start(), unroll),
            lambda: each(count, me, lambda k: copy(k, k).wait_recv(), unroll),
            lambda: each(count, me, lambda k: copy(k, me).wait_send(), False),
        )

    barrier = pltpu.get_barrier_semaphore()
    for count, me, device in ((slabs, slab, at_slab), (GROUP, g, at_group), (copies, r, at_copy)):
        each(count, me, lambda k, device=device: pl.semaphore_signal(
            barrier, inc=1, device_id=device(k), device_id_type=MESH))
    def volume_copy(k, again):
        return pltpu.make_async_copy(
            v_hbm.at[k], v_ref.at[pl.ds(pl.multiple_of(2 * depth * k + depth * again, depth), depth)], s_volume.at[again, k])

    loads = [
        pltpu.make_async_copy(source, target, s_load.at[k])
        for k, (source, target) in enumerate((
            (s_hbm, s_ref), (single_hbm, single), (down_hbm, down_ref), (across_hbm, across_ref), (up_hbm, up_ref),
            (low_hbm, low_ref), (high_hbm, high_ref), (shift_hbm, shift_ref)))
    ]

    def over(count, act):
        def step(k, carry):
            act(k)
            return carry

        lax.fori_loop(0, count, step, 0)

    for load in loads[5:]:
        load.start()
    for again in range(2):
        over(16, lambda k, again=again: volume_copy(k, again).start())
    for load in loads[:5]:
        load.start()
    for load in loads[5:]:
        load.wait()
    for again in range(2):
        over(16, lambda k, again=again: volume_copy(k, again).wait())
    begins = [item * 16 * depth + depth - shift_ref[item, 1] for item in range(2)]

    def fill(first, number, power):
        def step(t, power):
            for k in range(number):
                for item in range(2):
                    rows = v_ref[pl.ds(begins[item] + t * 8 + first + k, 8, stride=2 * depth), :]
                    u_ref[t, first + k, item] = rows
                    power = power + rows * rows
            return power

        return lax.fori_loop(0, slabs, step, power)

    powers = exchange(
        slabs, slab, at_slab, lambda k: power_out.at[0:1], lambda k: power_in.at[k, 0:1], s_power, r_power)
    block = exchange(slabs, slab, at_slab, lambda k: blocks.at[k], lambda k: block_in.at[k], s_block, r_block)
    tilt = exchange(GROUP, g, at_group, lambda k: tilt_out.at[0:2], lambda k: tilt_in.at[k, 0:2], s_tilt, r_tilt)
    tilts = exchange(copies, r, at_copy, lambda k: tilts_out, lambda k: tilts_in.at[k], s_tilts, r_tilts)
    own = exchange(copies, r, at_copy, lambda k: own_out, lambda k: own_in.at[k], s_own, r_own)
    chips, chip, core = slabs // 2, lax.div(slab, 2), lax.rem(slab, 2)
    around = sorted(range(chips), key=lambda d: min(d, chips - d))

    def piece(place, there):
        target = lax.rem(chip + around[place], chips) * 2 + there
        slot = around.index((chips - around[place]) % chips) * 2 + core
        return pltpu.make_async_remote_copy(
            src_ref=plane.at[pl.ds(pl.multiple_of(target * 8, 8), 8)], dst_ref=pieces_in.at[slot],
            send_sem=s_piece.at[place * 2 + there], recv_sem=r_piece.at[slot], device_id=at_slab(target), device_id_type=MESH)

    def pieces(act, places):
        for place in places:
            for there in ((1 - core,) if place == 0 else (0, 1)):
                act(place, there)

    def piece_wait(place, there):
        pltpu.make_async_remote_copy(
            src_ref=plane.at[0:8], dst_ref=pieces_in.at[place * 2 + there], send_sem=s_piece.at[place * 2 + there],
            recv_sem=r_piece.at[place * 2 + there], device_id=at_slab(slab), device_id_type=MESH).wait_recv()

    def whole_copy(batch_of, k, slot):
        cut = slice(batch_of[0] * 2, batch_of[1] * 2)
        at = batches.index(batch_of)
        return pltpu.make_async_remote_copy(
            src_ref=pieces_in.at[cut], dst_ref=planes_in.at[slot, cut], send_sem=s_plane.at[at, k], recv_sem=r_plane.at[at, slot],
            device_id=at_group(k), device_id_type=MESH)

    batches = [cut for cut in BATCHES if cut[1] <= chips] or [(0, chips)]

    def rows(c):
        first, number = lax.rem(x + 1 + c, XS) * 2, 2
        if c >= XS - 1:
            first, number = x * 2 + (1 - p if c == XS - 1 else p), 1
        return first, number, exchange(
            slabs, slab, at_slab, lambda k: u_ref.at[k, pl.ds(first, number)],
            lambda k: rows_in.at[pl.ds(first, number), :, k], s_rows.at[c], r_rows.at[c])

    def part_copy(k):
        return pltpu.make_async_remote_copy(
            src_ref=part.at[k], dst_ref=parts_in.at[g], send_sem=s_part.at[k], recv_sem=r_part.at[g],
            device_id=at_group(k), device_id_type=MESH)

    def part_wait(k):
        return pltpu.make_async_remote_copy(
            src_ref=part.at[k], dst_ref=parts_in.at[k], send_sem=s_part.at[k], recv_sem=r_part.at[k],
            device_id=at_group(k), device_id_type=MESH)

    def sums_over(turn):
        return exchange(
            GROUP, g, at_group, lambda k: some_out.at[turn, 0:1], lambda k: some_in.at[turn, k, 0:1], s_some.at[turn], r_some.at[turn],
        ), exchange(
            slabs, slab, at_slab, lambda k: more_out.at[turn, 0:1], lambda k: more_in.at[turn, k, 0:1], s_more.at[turn], r_more.at[turn])

    power = jnp.zeros((8, LANES), F32)
    for c in range(CHUNKS):
        first, number, moved = rows(c)
        power = fill(first, number, power)
        if c == 0:
            pl.semaphore_wait(barrier, slabs - 1 + GROUP - 1 + copies - 1)
        if c < 1:
            moved[0]()
    power_out[0:1] = jnp.sum(power, axis=0, keepdims=True)
    powers[0]()
    for c in range(1, CHUNKS):
        rows(c)[2][0]()
    loads[0].wait()

    def cut(t, carry):
        blocks[t] = s_ref[pl.ds(t * 8 + g, 8, stride=depth), :]
        return carry

    lax.fori_loop(0, slabs, cut, 0)
    block[0]()
    block_in[slab] = blocks[slab]
    power_in[slab, 0:1] = power_out[0:1]
    for k in range(8):
        for item in range(2):
            rows_in[k, item, slab] = u_ref[slab, k, item]

    lane = lax.broadcasted_iota(jnp.int32, (half, LANES), 1)
    row = lax.broadcasted_iota(jnp.int32, (half, LANES), 0)
    here = lane % HALF == row
    left = lane < HALF
    tile_row = lax.broadcasted_iota(jnp.int32, (8, LANES), 0)
    wide = lax.broadcasted_iota(jnp.int32, (tall, LANES), 1)

    spot = lax.broadcasted_iota(jnp.int32, (8, LANES), 1)
    edge = jnp.where(spot == 0, low_ref[0].astype(F32), jnp.where(spot == 1, low_ref[1].astype(F32), 0.0))
    edge = jnp.where(spot == 2, -high_ref[0].astype(F32), jnp.where(spot == 3, -high_ref[1].astype(F32), edge))
    edge = jnp.exp(edge * (1 / SOFTNESS))
    loads[1].wait()

    def table(k):
        return single[k * tall : (k + 1) * tall]

    def weight(p_table, q_table, low, high):
        return 1.0 / ((1.0 + p_table * high) * (1.0 + q_table * low))

    for item in range(2):
        low, high = edge[0:1, item : item + 1], edge[0:1, item + 2 : item + 3]
        w = weight(table(0), table(1), low, high)
        dw = weight(table(2), table(3), low, high) - w
        pick = wide == shift_ref[item, 0]
        zc = jnp.sum(jnp.where(pick, table(4), 0.0), axis=1, keepdims=True)
        zs = jnp.sum(jnp.where(pick, table(5), 0.0), axis=1, keepdims=True)
        first = 6 * tall + depth + 8
        xc = single[pl.ds(first + shift_ref[item, 2], 1), :]
        xs = single[pl.ds(first + LANES + shift_ref[item, 2], 1), :]
        cosine, sine = zc * xc - zs * xs, zs * xc + zc * xs
        factors[item, 0], factors[item, 1] = w * cosine, w * sine
        factors[item, 2], factors[item, 3] = dw * cosine, dw * sine

    powers[1]()
    energy = power_in[0, 0:1]
    for k in range(1, slabs):
        energy = energy + power_in[k, 0:1]
    tilt_out[0:1] = edge[0:1]
    tilt_out[1:2] = energy
    tilt[0]()
    tilt_in[g, 0:2] = tilt_out[0:2]
    for load in loads[2:5]:
        load.wait()
    down, across, up = down_ref[...], across_ref[...], up_ref[...]

    def chunk(c):
        first, number, moved = rows(c)
        moved[1]()
        stack = []
        for k in range(number):
            for item in range(2):
                stack.append(table_by(down, rows_in[first + k, item].reshape(depth, LANES)))
        product = by_table(jnp.concatenate(stack, 0), across)
        for k in range(number):
            re = im = re_last = im_last = d_re = d_im = 0.0
            for item in range(2):
                at = (k * 2 + item) * (depth + 8)
                c_top, c_low, c_last = (product[at + a : at + b, :LANES] for a, b in ((0, half), (half, depth), (depth, depth + 8)))
                s_top, s_low, s_last = (product[at + a : at + b, LANES:] for a, b in ((0, half), (half, depth), (depth, depth + 8)))
                a, b = c_top + s_low, c_low - s_top
                wc, ws = factors[item, 0, :half], factors[item, 1, :half]
                re, im = re + wc * a + ws * b, im + wc * b - ws * a
                wc, ws = factors[item, 2, :half], factors[item, 3, :half]
                d_re, d_im = d_re + wc * a + ws * b, d_im + wc * b - ws * a
                wc, ws = factors[item, 0, half:], factors[item, 1, half:]
                re_last, im_last = re_last + wc * c_last - ws * s_last, im_last - wc * s_last - ws * c_last

            def lying(d):
                column = jnp.where(left, d[:, 0:1], d[:, HALF : HALF + 1])
                return jnp.sum(jnp.where(here, column, 0.0), axis=0, keepdims=True)

            last = jnp.where(tile_row == 0, re_last[0:1], jnp.where(tile_row == 1, im_last[0:1], 0.0))
            last = jnp.where(tile_row == 2, lying(d_re), jnp.where(tile_row == 3, lying(d_im), last))
            part[first + k, 0:half], part[first + k, half:depth] = re, im
            part[first + k, depth:] = last
        return first

    def add_up(ref, count):
        total = ref[0]
        for k in range(1, count):
            total = total + ref[k]
        return total

    for c in range(CHUNKS):
        first = chunk(c)
        if c < XS - 1:
            part_copy(first + 1 - p).start()
            part_copy(first + p).start()
        elif c == XS - 1:
            part_copy(first).start()
        if c == 0:
            tilt[1]()
            tilts_out[0:8] = jnp.concatenate([tilt_in[k, 0:1] for k in range(GROUP)], 0)
            energy = tilt_in[0, 1:2]
            for k in range(1, GROUP):
                energy = energy + tilt_in[k, 1:2]
            tilts_out[8:16] = jnp.broadcast_to(energy, (8, LANES))
            tilts[0]()
            tilts_in[r] = tilts_out[...]
        if c == 2:
            tilts[1]()
            energy = tilts_in[0, 8:9]
            for k in range(1, copies):
                energy = energy + tilts_in[k, 8:9]

            def square(k, totals):
                total, mirrored = totals
                for j in range(GROUP):
                    for item in range(2):
                        low, high = tilts_in[k, j : j + 1, item : item + 1], tilts_in[k, j : j + 1, item + 2 : item + 3]
                        w = weight(table(0), table(1), low, high)
                        total = total + w * w
                        w = weight(table(2), table(3), low, high)
                        mirrored = mirrored + w * w
                return total, mirrored

            none = jnp.zeros((tall, LANES), F32)
            total, mirrored = lax.fori_loop(0, copies, square, (none, none))

    parts_in[g] = part[g]
    each(GROUP, g, lambda k: part_wait(k).wait_recv())
    own_out[...] = add_up(parts_in, GROUP)
    own[0]()
    own_in[r] = own_out[...]

    def stacked(d):
        return jnp.concatenate([d[:half], d[:half], jnp.where(tile_row < 2, d[half : half + 1], 0.0)], 0)

    d_one, d_two = stacked(total), stacked(mirrored)
    block[1]()
    support = block_in[...].reshape(depth, LANES)
    sign = jnp.where(lax.broadcasted_iota(jnp.int32, (depth, LANES), 0) % 2 == 0, 1.0, -1.0) * (1 / math.sqrt(depth))
    count = single[6 * tall : 6 * tall + depth + 8]
    powers[2](), block[2](), tilt[2](), tilts[2]()
    for c in range(CHUNKS):
        rows(c)[2][2]()
    own[1]()
    sums = add_up(own_in, copies)

    def standing(values):
        spread = jnp.where(here, values, 0.0)
        one = jnp.sum(jnp.where(left, spread, 0.0), axis=1, keepdims=True)
        two = jnp.sum(jnp.where(left, 0.0, spread), axis=1, keepdims=True)
        return jnp.where(lane == 0, one, jnp.where(lane == HALF, two, 0.0))

    change = jnp.concatenate(
        [standing(sums[depth + 2 : depth + 3]), standing(sums[depth + 3 : depth + 4]), jnp.zeros((8, LANES), F32)], 0)
    sums = jnp.concatenate([sums[:depth], jnp.where(tile_row < 2, sums[depth:], 0.0)], 0)
    mean = jnp.zeros((depth + 8, LANES), F32)
    power = jnp.sum(energy, axis=(0, 1), keepdims=True)
    misfit = power * (1.0 / (subs * cells))
    misfits = [misfit]
    for turn in range(ITERS):
        damping = REG_WEIGHT * subs * misfit + FLOOR_VALUE
        one, two = 0.5 / (d_one + damping), 0.5 / (d_two + damping)
        update = mean - mean * (d_one * one + d_two * two) + (one + two) * sums + two * change
        product = by_table(update, across)
        re = product[:half, :LANES] - product[half:depth, LANES:]
        im = product[half:depth, :LANES] + product[:half, LANES:]
        last = product[depth : depth + 1, :LANES] - product[depth + 1 : depth + 2, LANES:]
        field = table_by(up, jnp.concatenate([re, im], 0)) + sign * last
        if turn + 1 == ITERS:
            break
        product = by_table(table_by(down, support * field), across)
        last = jnp.where(tile_row == 0, product[depth : depth + 1, :LANES], -product[depth : depth + 1, LANES:])
        mean = jnp.concatenate([
            product[:half, :LANES] + product[half:depth, LANES:],
            product[half:depth, :LANES] - product[:half, LANES:],
            jnp.where(tile_row < 2, last, 0.0)], 0)
        terms = count * mean * (0.5 * (d_one + d_two) * mean - 2.0 * sums - change)
        some_out[turn, 0:1] = jnp.sum(terms, axis=0, keepdims=True)
        some, more = sums_over(turn)
        some[0]()
        some_in[turn, g, 0:1] = some_out[turn, 0:1]
        if turn == 0:
            own[2]()
            each(GROUP, g, lambda k: part_wait(k).wait_send(), False)
        some[1]()
        more_out[turn, 0:1] = add_up(some_in.at[turn, :, 0:1], GROUP)
        more[0]()
        more_in[turn, slab, 0:1] = more_out[turn, 0:1]
        more[1]()
        misfit = (power + jnp.sum(add_up(more_in.at[turn, :, 0:1], slabs), axis=(0, 1), keepdims=True)) * (1.0 / (subs * cells))
        misfits.append(misfit)
    plane[...] = field
    pieces(lambda place, there: piece(place, there).start(), range(chips))
    pieces_in[core] = plane[pl.ds(pl.multiple_of(slab * 8, 8), 8)]

    def place(k, source, cut):
        for at in range(*cut):
            for there in range(2):
                j = lax.rem(chip + around[at], chips) * 2 + there
                out_ref[pl.ds(j * 8 + k, 8, stride=depth), :] = source[at * 2 + there]

    for cut in batches:
        pieces(piece_wait, range(*cut))
        each(GROUP, g, lambda k: whole_copy(cut, k, g).start())
    for turn in range(ITERS):
        mis_ref[turn] = jnp.sum(misfits[turn])
    for turn in range(ITERS - 1):
        sums_over(turn)[0][2](), sums_over(turn)[1][2]()
    pieces(lambda place, there: piece(place, there).wait_send(), range(chips))
    for cut in batches:
        place(g, pieces_in, cut)

        def arrived(k):
            whole_copy(cut, k, k).wait_recv()
            place(k, planes_in.at[k], cut)

        each(GROUP, g, arrived)
    for cut in batches:
        each(GROUP, g, lambda k: whole_copy(cut, k, g).wait_send())


def body(volumes, tilt_low, tilt_high, shifts, support):
    slabs, ring = lax.axis_size("slab"), lax.axis_size("batch") // XS
    layer, ys, width = support.shape
    depth, copies, tall = layer * slabs, ring // 2, slabs * 8 + 8
    vmem, smem, hbm = (pl.BlockSpec(memory_space=space) for space in (pltpu.VMEM, pltpu.SMEM, pl.ANY))
    down, across, up, single = (jnp.asarray(table) for table in tables(depth, width))
    dma = pltpu.SemaphoreType.DMA

    def buffer(*shape):
        return pltpu.VMEM((*shape, LANES), F32)

    field, misfits = pl.pallas_call(
        functools.partial(refine, slabs, ring),
        out_shape=(pltpu.VMEM((layer * ys, width), F32), jax.ShapeDtypeStruct((ITERS,), F32)),
        in_specs=[hbm] * 9,
        out_specs=(vmem, smem),
        scratch_shapes=[
            pltpu.SMEM((2,), jnp.int32), pltpu.SMEM((2,), jnp.int32), pltpu.SMEM((2, 3), jnp.int32),
            buffer(2 * layer * 2 * ys), buffer(layer * ys), pltpu.VMEM(down.shape, BF16), pltpu.VMEM(across.shape, BF16),
            pltpu.VMEM(up.shape, BF16), buffer(single.shape[0]), buffer(slabs, 8, 2, 8), buffer(slabs, 8),
            buffer(8), buffer(slabs, 8), buffer(slabs, 8), buffer(8), buffer(GROUP, 8), buffer(16), buffer(copies, 16),
            buffer(8, 2, slabs, 8), buffer(2, 4, depth // 2 + 8),
            buffer(GROUP, tall), buffer(GROUP, tall), buffer(tall), buffer(copies, tall),
            buffer(2, 8), buffer(2, GROUP, 8), buffer(2, 8), buffer(2, slabs, 8),
            buffer(depth), buffer(slabs, 8), buffer(GROUP, slabs, 8), dma((8,)), dma((2, 16)),
            dma((slabs,)), dma((slabs,)), dma((slabs,)), dma((slabs,)), dma((GROUP,)), dma((GROUP,)), dma((copies,)), dma((copies,)),
            dma((CHUNKS, slabs)), dma((CHUNKS, slabs)), dma((GROUP,)), dma((GROUP,)), dma((copies,)), dma((copies,)),
            dma((2, GROUP)), dma((2, GROUP)), dma((2, slabs)), dma((2, slabs)),
            dma((slabs,)), dma((slabs,)), dma((3, GROUP)), dma((3, GROUP)),
        ],
        compiler_params=pltpu.CompilerParams(collective_id=0, has_side_effects=True),
        name="refine",
    )(volumes.reshape(2 * layer, ys, width), support.reshape(layer * ys, width), down, across, up, single, tilt_low, tilt_high, shifts)
    return support * field.reshape(layer, ys, width), misfits


def solution(mesh):
    placed = (
        P("batch", "slab", None, None),
        P("batch"),
        P("batch"),
        P("batch", None),
        P("slab", None, None),
    )
    return jax.shard_map(
        body, mesh=mesh, in_specs=placed, out_specs=(P("slab", None, None), P()), check_vma=False
    )
```
